32 devices in a mesh: pts: 8 (over y, x, core), cand: 4 (over z).
Axes of the slice: x: 2, y: 2, z: 4, core: 2. Of those that a mesh axis runs over, the one named last changes fastest.
Arguments:
- points: bfloat16 [8192, 1024], P('pts'), may hold values from -6 to 6
- weights: float32 [8192], P('pts'), may hold values from 0.5 to 5
- coverage: float32 [8192], P('pts'), may hold values from -0.5 to 1
- candidates: bfloat16 [4096, 1024], P('cand'), may hold values from -6 to 6
- picks: int32 [64], replicated, may hold values from 0 to 4095
Outputs:
- gains: float32 [4096], P('cand')
- top_gains: float32 [64], replicated
- new_coverage: float32 [8192], P('pts')
The draws below stay inside these ranges and needn't reach their ends.
All inputs are finite; a program needn't handle non-finite values.
Results may differ from the reference program's by a relative error of at most 0.0003.
Values may be sent and summed in bfloat16 or wider, within the bound.
A program may use at most 64 MiB of HBM per device.

```python
import math
import jax
import jax.numpy as jnp
from jax import lax

D = 1024
CAND_DEV = 1024
NPICK = 64
TOPK = 64
NPTS = 8192
NCAND = 4096
N_CAND = 4


def set_ends(result, rng, smallest, top_value):
    dims = result.shape
    place = [jax.random.randint(jax.random.fold_in(rng, axis), (), 0, dims[axis]) for axis in range(len(dims))]
    result = result.at[tuple(place)].set(smallest)
    longest = dims.index(max(dims))
    place[longest] = (place[longest] + 1) % dims[longest]
    return result.at[tuple(place)].set(top_value)


def block_levels(stream_key, dims, shards, smallest, largest):
    def one(position, parts):
        heights = jax.random.uniform(jax.random.fold_in(jax.random.fold_in(stream_key, 6), position), (parts,), jnp.float32, smallest / len(shards), largest / len(shards))
        return jnp.repeat(jnp.exp(heights), dims[position] // parts).reshape((-1,) + (1,) * (len(dims) - position - 1))

    gain = one(*shards[0])
    for cut in shards[1:]:
        gain = gain * one(*cut)
    return gain


def noise(key, shape, width, most, shards=(), dtype=jnp.bfloat16):
    entries = jax.random.normal(key, shape, jnp.float32) * width
    if len(shards) > 0:
        entries = block_levels(key, shape, shards, -0.22, 0.18) * entries
    return jnp.clip(entries, min=-most, max=most).astype(dtype)


def setup_inputs(seed: int = 0) -> dict:
    key_of = jax.random.split(jax.random.key(seed), 6)
    return {
        "points": noise(key_of[0], (NPTS, D), 1.0, 6.0, ((0, 8),)),
        "weights": jnp.clip(jnp.exp(math.log(5.0) - 2.3025851 * jax.random.uniform(key_of[1], (NPTS,), jnp.float32) ** block_levels(key_of[1], (NPTS,), ((0, 8),), -0.2, 0.2)), 0.5, 5.0),
        "coverage": jnp.clip(-0.5 + 1.5 * jax.random.uniform(key_of[2], (NPTS,), jnp.float32) ** block_levels(key_of[2], (NPTS,), ((0, 8),), -0.2, 0.2), -0.5, 1.0),
        "candidates": noise(key_of[3], (NCAND, D), 1.0, 6.0, ((0, 4),)),
        "picks": set_ends(jax.random.randint(key_of[4], (NPICK,), 0, NCAND), jax.random.fold_in(key_of[4], 1), 0, NCAND - 1).astype(jnp.int32),
    }


def reference(points, weights, coverage, candidates, picks):
    scale = D ** -0.5
    total = points.shape[0]
    blocks = candidates.reshape(N_CAND, CAND_DEV, D)

    def block_gain(block):
        sims = jnp.dot(points, block.T, preferred_element_type=jnp.float32) * scale
        return jnp.sum(weights[:, None] * jnp.maximum(sims - coverage[:, None], 0.0), axis=0) / total

    gains = lax.map(block_gain, blocks).reshape(-1)
    top_gains = lax.top_k(gains, TOPK)[0]
    picked = jnp.take(candidates, picks.astype(jnp.int32), axis=0)
    picked_sims = jnp.dot(points, picked.T, preferred_element_type=jnp.float32) * scale
    new_coverage = jnp.maximum(coverage, jnp.max(picked_sims, axis=1))
    return gains, top_gains, new_coverage
```

```python
import functools

import jax
import jax.numpy as jnp
from jax import lax
from jax.experimental import pallas as pl
from jax.experimental.pallas import tpu as pltpu
from jax.sharding import PartitionSpec as P

TOPK = 64
LANES = 128
MESH = pl.DeviceIdType.MESH
F32 = jnp.float32
LOW = -1e30
HIGH = 3e38
HALF = 512
WIDE = 256
STEP = 64


def column_tile(row):
    return jnp.transpose(jnp.broadcast_to(row, (LANES, LANES)))


def kernel(
    n_pts, n_cand, points, weights, coverage, candidates, picks, gains_out, top_out, cover_out,
    p_buf, c_buf, w_buf, v_buf, k_buf, w_col, v_col, b_acc, part_a, part_b, parts_a, parts_b,
    best, bests, all_gains, n_col, t_col, top_row, got_gains, got_top,
    in_sem, small_sem, a_send, a_recv, b_send, b_recv, best_send, best_recv,
    gain_send, gain_recv, top_send, top_recv, sent,
):
    rows, depth = points.shape
    cands = candidates.shape[0]
    me, mz = lax.axis_index("pts"), lax.axis_index("cand")
    n_p, n_c = rows // HALF, cands // WIDE
    tiles_p, tiles_c = rows // LANES, cands // LANES
    tiles_w = WIDE // LANES
    rows_b = tiles_w
    rows_a = tiles_c - rows_b
    pair = 2 if n_pts % 2 == 0 else 1
    scale = depth ** (-0.5)

    loads = {}
    order = [("c", 0), ("p", 0)] + [("p", i) for i in range(1, n_p)] + [("c", i) for i in range(1, n_c)]
    for at, (kind, i) in enumerate(order):
        src, dst, size = (points, p_buf, HALF) if kind == "p" else (candidates, c_buf, WIDE)
        span = pl.ds(i * size, size)
        loads[kind, i] = pltpu.make_async_copy(src.at[span, :], dst.at[span, :], in_sem.at[at])
    small = [
        pltpu.make_async_copy(weights, w_buf, small_sem.at[0]),
        pltpu.make_async_copy(coverage, v_buf, small_sem.at[1]),
        pltpu.make_async_copy(picks, k_buf, small_sem.at[2]),
    ]
    for copy in small:
        copy.start()
    for key in order:
        loads[key].start()

    base = mz == 0
    relay = me // pair * pair + pair - 1
    speaks = base & (me == relay)
    barrier = pltpu.get_barrier_semaphore()

    def greet(p, z):
        pl.semaphore_signal(barrier, inc=1, device_id={"pts": p, "cand": z}, device_id_type=MESH)

    @pl.when(base)
    def _():
        for z in range(n_cand):
            for k in range(n_pts):
                if z == 0 and k == 0:
                    continue
                greet(lax.rem(me + k, n_pts), z)

    for k in range(1, n_cand):
        greet(me, lax.rem(mz + k, n_cand))

    @pl.when(jnp.logical_not(base))
    def _():
        greet(relay, 0)

    for copy in small:
        copy.wait()
    w_row = w_buf[...] * (scale / (rows * n_pts))
    v_row = v_buf[...] * (1.0 / scale)
    for t in range(tiles_p):
        w_col[t * LANES : (t + 1) * LANES, :] = column_tile(w_row[t : t + 1, :])
        v_col[t * LANES : (t + 1) * LANES, :] = column_tile(v_row[t : t + 1, :])
    column = mz * cands + lax.broadcasted_iota(jnp.int32, (tiles_c, LANES), 0) * LANES
    column = column + lax.broadcasted_iota(jnp.int32, (tiles_c, LANES), 1)
    chosen = jnp.zeros((tiles_c, LANES), jnp.bool_)
    for k in range(picks.shape[0]):
        chosen = chosen | (column == k_buf[k])
    penalty = jnp.where(chosen, 0.0, LOW)

    def dot(p_from, many, c):
        return lax.dot_general(
            p_buf[p_from : p_from + many, :], c_buf[c * WIDE : (c + 1) * WIDE, :],
            (((1,), (1,)), ((), ())), preferred_element_type=F32,
        )

    def epilogue(sims, p_from, c, sums):
        many = sims.shape[0]
        for r in range(0, many, STEP):
            at = slice(p_from + r, p_from + r + STEP)
            w, v = w_col[at, :], v_col[at, :]
            found = b_acc[at, :] if c else None
            for t in range(tiles_w):
                x = sims[r : r + STEP, t * LANES : (t + 1) * LANES]
                value = jnp.maximum(x - v, 0.0) * w
                value = jnp.sum(value.reshape(STEP // 8, 8, LANES), axis=0)
                sums[t] = value if sums[t] is None else sums[t] + value
                tile = c * tiles_w + t
                x = x + penalty[tile : tile + 1, :]
                found = x if found is None else jnp.maximum(found, x)
            b_acc[at, :] = found

    def settle_sums(sums, dst, c):
        for t in range(tiles_w):
            dst[c * tiles_w + t : c * tiles_w + t + 1, :] = jnp.sum(sums[t], axis=0, keepdims=True)

    def send_parts(src, slots, send, recv):
        def to(p):
            pltpu.make_async_remote_copy(
                src_ref=src, dst_ref=slots.at[mz, me], send_sem=send.at[0], recv_sem=recv.at[mz],
                device_id={"pts": p, "cand": 0}, device_id_type=MESH,
            ).start()

        @pl.when(jnp.logical_not(base))
        def _():
            for p in range(n_pts):
                to(p)

        @pl.when(base)
        def _():
            for k in range(1, n_pts):
                to(lax.rem(me + k, n_pts))
            slots[0, me] = src[...]

    work = []
    for i in range(n_p):
        work.append((i * HALF, HALF, 0, ("p", i)))
    for c in range(1, n_c):
        work.append((0, rows, c, ("c", c)))
    loads["c", 0].wait()
    sums = [None] * tiles_w
    held = None
    for at, (p_from, many, c, key) in enumerate(work):
        loads[key].wait()
        sims = dot(p_from, many, c)
        if held is not None:
            epilogue(*held, sums)
            if held[2] != c:
                settle_sums(sums, part_a, held[2])
                sums = [None] * tiles_w
        held = (sims, p_from, c)

    greetings = (n_cand - 1) + n_pts
    awaited = jnp.where(base, greetings - 1, greetings)
    awaited = awaited + jnp.where(speaks, pair * (n_cand - 1), 0)
    pl.semaphore_wait(barrier, awaited)
    send_parts(part_a, parts_a, a_send, a_recv)
    epilogue(*held, sums)
    settle_sums(sums, part_b, 0)
    send_parts(part_b, parts_b, b_send, b_recv)

    for t in range(tiles_p):
        turned = jnp.transpose(b_acc[t * LANES : (t + 1) * LANES, :])
        best[t : t + 1, :] = jnp.max(turned, axis=0, keepdims=True)
    for k in range(1, n_cand):
        pltpu.make_async_remote_copy(
            src_ref=best, dst_ref=bests.at[mz], send_sem=best_send.at[0], recv_sem=best_recv.at[0],
            device_id={"cand": lax.rem(mz + k, n_cand)}, device_id_type=MESH,
        ).start()

    def settle(view, sem):
        pltpu.make_async_copy(view, view, sem).wait()

    def finish_cover():
        settle(bests.at[pl.ds(0, n_cand - 1)], best_recv.at[0])
        cover = best[...]
        for k in range(1, n_cand):
            cover = jnp.maximum(cover, bests[lax.rem(mz + k, n_cand)])
        cover_out[...] = jnp.maximum(v_buf[...], cover * scale)
        settle(bests.at[pl.ds(0, n_cand - 1)], best_send.at[0])

    place = lax.broadcasted_iota(jnp.int32, (8, LANES), 1).astype(F32)
    lane = lax.broadcasted_iota(jnp.int32, (1, LANES), 1)

    def merge(new):
        for i, row in enumerate(new):
            n_col[i * LANES : (i + 1) * LANES, :] = column_tile(row)
        across = [jnp.broadcast_to(row, (8, LANES)) for row in new]
        across.append(jnp.broadcast_to(top_row[...], (8, LANES)))
        columns = [t_col[g * 8 : (g + 1) * 8, :] for g in range(TOPK // 8)]
        columns += [n_col[g * 8 : (g + 1) * 8, :] for g in range(len(new) * LANES // 8)]
        kept = jnp.full((8, LANES), HIGH, F32)
        for column in columns:
            above = jnp.zeros((8, LANES), F32)
            for row in across:
                above = above + jnp.where(row > column, 1.0, 0.0)
            above = jnp.sum(above, axis=1, keepdims=True)
            kept = jnp.minimum(kept, jnp.where(above <= place, column, HIGH))
        kept = jnp.min(kept, axis=0, keepdims=True)
        return jnp.where(lane < TOPK, kept, LOW)

    def told(z, k, src, dst, send, recv):
        return pltpu.make_async_remote_copy(
            src_ref=src, dst_ref=dst, send_sem=send.at[0], recv_sem=recv.at[0],
            device_id={"pts": me - pair + 1 + k, "cand": z}, device_id_type=MESH,
        )

    @pl.when(base)
    def _():
        top_row[...] = jnp.where(lane < TOPK, -1.0, LOW)
        for z in range(n_cand):
            count = n_pts - 1 if z == 0 else n_pts
            for slots, recv, first, many in (
                (parts_a, a_recv, 0, rows_a), (parts_b, b_recv, rows_a, rows_b)
            ):
                t_col[...] = column_tile(top_row[...])[:TOPK, :]
                settle(slots.at[0, pl.ds(0, count)], recv.at[z])
                total = slots[z, 0]
                for p in range(1, n_pts):
                    total = total + slots[z, p]
                all_gains[z, first : first + many, :] = total
                top_row[...] = merge([total[t : t + 1, :] for t in range(many)])
            if z:
                @pl.when(speaks)
                def _():
                    for k in range(pair):
                        told(z, k, all_gains.at[z], got_gains, gain_send, gain_recv).start()
            if z == n_cand - 2:
                finish_cover()
                gains_out[...] = all_gains[0]
                settle(parts_a.at[0, pl.ds(0, n_pts - 1)], a_send.at[0])
                settle(parts_b.at[0, pl.ds(0, n_pts - 1)], b_send.at[0])
        top_out[...] = top_row[:, :TOPK]

        @pl.when(speaks)
        def _():
            for z in range(1, n_cand):
                for k in range(pair):
                    told(z, k, top_row, got_top, top_send, top_recv).start()
            many = pair * (n_cand - 1)
            for k in range(many):
                settle(got_gains, gain_send.at[0])
                settle(got_top, top_send.at[0])

    @pl.when(jnp.logical_not(base))
    def _():
        finish_cover()
        settle(parts_a.at[0, pl.ds(0, n_pts)], a_send.at[0])
        settle(parts_b.at[0, pl.ds(0, n_pts)], b_send.at[0])
        settle(got_gains, gain_recv.at[0])
        gains_out[...] = got_gains[...]
        settle(got_top, top_recv.at[0])
        top_out[...] = got_top[:, :TOPK]


def finish(gains, top, cover, gains_out, top_out, cover_out, sems):
    copies = [
        pltpu.make_async_copy(top, top_out, sems.at[0]),
        pltpu.make_async_copy(gains, gains_out, sems.at[1]),
        pltpu.make_async_copy(cover, cover_out, sems.at[2]),
    ]
    for copy in copies:
        copy.start()
    for copy in copies:
        copy.wait()


def solution(mesh):
    n_pts, n_cand = mesh.shape["pts"], mesh.shape["cand"]

    def on_device(points, weights, coverage, candidates, picks):
        rows, depth = points.shape
        cands = candidates.shape[0]
        tp, tc = rows // LANES, cands // LANES
        tb = WIDE // LANES
        ta = tc - tb
        anywhere = pl.BlockSpec(memory_space=pl.ANY)
        dma = pltpu.SemaphoreType.DMA
        vmem = pltpu.VMEM
        gains, top, cover = pl.pallas_call(
            functools.partial(kernel, n_pts, n_cand),
            out_shape=(vmem((tc, LANES), F32), vmem((1, TOPK), F32), vmem((tp, LANES), F32)),
            in_specs=[anywhere] * 5,
            out_specs=(pl.BlockSpec(memory_space=vmem),) * 3,
            scratch_shapes=[
                vmem((rows, depth), points.dtype), vmem((cands, depth), candidates.dtype),
                vmem((tp, LANES), F32), vmem((tp, LANES), F32),
                pltpu.SMEM(picks.shape, jnp.int32),
                vmem((rows, LANES), F32), vmem((rows, LANES), F32), vmem((rows, LANES), F32),
                vmem((ta, LANES), F32), vmem((tb, LANES), F32),
                vmem((n_cand, n_pts, ta, LANES), F32), vmem((n_cand, n_pts, tb, LANES), F32),
                vmem((tp, LANES), F32), vmem((n_cand, tp, LANES), F32),
                vmem((n_cand, tc, LANES), F32), vmem((cands, LANES), F32), vmem((TOPK, LANES), F32),
                vmem((1, LANES), F32), vmem((tc, LANES), F32), vmem((1, LANES), F32),
                dma((rows // HALF + cands // WIDE,)), dma((3,)),
                dma((1,)), dma((n_cand,)), dma((1,)), dma((n_cand,)), dma((1,)), dma((1,)),
                dma((1,)), dma((1,)), dma((1,)), dma((1,)),
                vmem((2 * (n_cand - 1), tc, LANES), F32),
            ],
            compiler_params=pltpu.CompilerParams(
                collective_id=0, has_side_effects=True, vmem_limit_bytes=60 * 2**20
            ),
            name="facility",
        )(points, weights.reshape(tp, LANES), coverage.reshape(tp, LANES), candidates, picks)
        gains, top, cover = pl.pallas_call(
            finish,
            out_shape=(
                jax.ShapeDtypeStruct((tc, LANES), F32),
                jax.ShapeDtypeStruct((1, TOPK), F32),
                jax.ShapeDtypeStruct((tp, LANES), F32),
            ),
            in_specs=[pl.BlockSpec(memory_space=vmem)] * 3,
            out_specs=(anywhere,) * 3,
            scratch_shapes=[dma((3,))],
            name="finish",
        )(*(pltpu.with_memory_space_constraint(x, vmem) for x in (gains, top, cover)))
        return gains.reshape(cands), top.reshape(TOPK), cover.reshape(rows)

    placed = (P("pts", None), P("pts"), P("pts"), P("cand", None), P())
    return jax.shard_map(
        on_device, mesh=mesh, in_specs=placed, out_specs=(P("cand"), P(), P("pts")), check_vma=False
    )
```

```python
import functools

import jax
import jax.numpy as jnp
from jax import lax
from jax.experimental import pallas as pl
from jax.experimental.pallas import tpu as pltpu
from jax.sharding import PartitionSpec as P

TOPK = 64
LANES = 128
MESH = pl.DeviceIdType.MESH
F32 = jnp.float32
LOW = -1e30
HIGH = 3e38
WIDE = 256
PIECE = 64


def column_tile(row):
    return jnp.transpose(jnp.broadcast_to(row, (LANES, LANES)))


def kernel(
    n_pts, n_cand, points, weights, coverage, candidates, picks, gains_out, top_out, cover_out,
    p_buf, c_buf, w_buf, v_buf, k_buf, w_col, v_col, b_acc, last, part_a, part_b, parts_a, parts_b,
    best, bests, all_gains, n_col, t_col, top_row, got_gains, got_top,
    in_sem, small_sem, a_send, a_recv, b_send, b_recv, best_send, best_recv,
    gain_send, gain_recv, top_send, top_recv, *accs,
):
    rows, depth = points.shape
    cands = candidates.shape[0]
    me, mz = lax.axis_index("pts"), lax.axis_index("cand")
    n_k, n_c = depth // WIDE, cands // WIDE
    half = rows // 2
    pieces = half // PIECE
    tiles_p, tiles_c = rows // LANES, cands // LANES
    tiles_w = WIDE // LANES
    rows_b = tiles_w
    rows_a = tiles_c - rows_b
    pair = 2 if n_pts % 2 == 0 else 1
    scale = depth ** (-0.5)

    steps = [(c, k) for c in range(n_c) for k in range(n_k)]
    order = [("c", steps[0])]
    for at, step in enumerate(steps):
        if at + 1 < len(steps):
            order.append(("c", steps[at + 1]))
        if step[0] == 0:
            order.append(("p", step))
    loads = {}
    for at, (kind, (c, k)) in enumerate(order):
        side = pl.ds(k * WIDE, WIDE)
        if kind == "p":
            src, dst = points.at[:, side], p_buf.at[:, side]
        else:
            down = pl.ds(c * WIDE, WIDE)
            src, dst = candidates.at[down, side], c_buf.at[down, side]
        loads[kind, (c, k)] = pltpu.make_async_copy(src, dst, in_sem.at[at])
    small = [
        pltpu.make_async_copy(weights, w_buf, small_sem.at[0]),
        pltpu.make_async_copy(coverage, v_buf, small_sem.at[1]),
        pltpu.make_async_copy(picks, k_buf, small_sem.at[2]),
    ]
    for key in order[:3]:
        loads[key].start()
    for copy in small:
        copy.start()
    for key in order[3:]:
        loads[key].start()

    base = mz == 0
    relay = me // pair * pair + pair - 1
    speaks = base & (me == relay)
    barrier = pltpu.get_barrier_semaphore()

    def greet(p, z):
        pl.semaphore_signal(barrier, inc=1, device_id={"pts": p, "cand": z}, device_id_type=MESH)

    @pl.when(base)
    def _():
        for z in range(n_cand):
            for k in range(n_pts):
                if z == 0 and k == 0:
                    continue
                greet(lax.rem(me + k, n_pts), z)

    for k in range(1, n_cand):
        greet(me, lax.rem(mz + k, n_cand))

    @pl.when(jnp.logical_not(base))
    def _():
        greet(relay, 0)

    for copy in small:
        copy.wait()
    w_row = w_buf[...] * (scale / (rows * n_pts))
    v_row = v_buf[...] * (1.0 / scale)
    for t in range(tiles_p):
        w_col[t * LANES : (t + 1) * LANES, :] = column_tile(w_row[t : t + 1, :])
        v_col[t * LANES : (t + 1) * LANES, :] = column_tile(v_row[t : t + 1, :])
    column = mz * cands + lax.broadcasted_iota(jnp.int32, (tiles_c, LANES), 0) * LANES
    column = column + lax.broadcasted_iota(jnp.int32, (tiles_c, LANES), 1)
    chosen = jnp.zeros((tiles_c, LANES), jnp.bool_)
    for k in range(picks.shape[0]):
        chosen = chosen | (column == k_buf[k])
    penalty = jnp.where(chosen, 0.0, LOW)

    def push(at):
        c, k = steps[at]
        tile = c_buf[c * WIDE : (c + 1) * WIDE, k * WIDE : (k + 1) * WIDE]
        for q in range(2):
            pltpu.matmul_push_rhs(tile, staging_register=at % 2, mxu_index=q, transpose=True)

    def accumulator(c, i, q):
        return accs[((c % 2) * 2 + q) * pieces + i]

    def accumulate(at):
        c, k = steps[at]
        for i in range(pieces):
            for q in range(2):
                from_p = q * half + i * PIECE
                pltpu.matmul_acc_lhs(
                    accumulator(c, i, q),
                    p_buf[from_p : from_p + PIECE, k * WIDE : (k + 1) * WIDE],
                    load_staged_rhs=at % 2 if i == 0 else None,
                )

    sums = {}

    def gain_of(x, at, c, t):
        value = jnp.maximum(x - v_col[at, :], 0.0) * w_col[at, :]
        value = jnp.sum(value.reshape(PIECE // 8, 8, LANES), axis=0)
        sums[c, t] = sums[c, t] + value if (c, t) in sums else value

    def cover_of(xs, at, c):
        found = b_acc[at, :] if c else None
        for t, x in enumerate(xs):
            tile = c * tiles_w + t
            x = x + penalty[tile : tile + 1, :]
            found = x if found is None else jnp.maximum(found, x)
        b_acc[at, :] = found

    def consume(c, i, q):
        from_p = q * half + i * PIECE
        at = slice(from_p, from_p + PIECE)
        sims = pltpu.matmul_pop(accumulator(c, i, q))
        xs = [sims[:, t * LANES : (t + 1) * LANES] for t in range(tiles_w)]
        for t, x in enumerate(xs):
            gain_of(x, at, c, t)
        if c + 1 < n_c:
            cover_of(xs, at, c)
        else:
            last[at, :] = sims

    def write_sums(c, dst, row):
        for t in range(tiles_w):
            dst[row + t : row + t + 1, :] = jnp.sum(sums[c, t], axis=0, keepdims=True)

    def send_parts(src, slots, send, recv):
        slots[0, me] = src[...]
        for k in range(n_pts):
            p = k + jnp.where(base & (k >= me), 1, 0)
            copy = pltpu.make_async_remote_copy(
                src_ref=src, dst_ref=slots.at[mz, me], send_sem=send.at[0], recv_sem=recv.at[mz],
                device_id={"pts": p, "cand": 0}, device_id_type=MESH,
            )
            if k + 1 < n_pts:
                copy.start()
            else:
                pl.when(jnp.logical_not(base))(copy.start)

    loads["c", steps[0]].wait()
    push(0)
    units = [(i, q) for i in range(pieces) for q in range(2)]
    share = len(units) // n_k
    for at, (c, k) in enumerate(steps):
        if c == 0:
            loads["p", (c, k)].wait()
        if at + 1 < len(steps):
            loads["c", steps[at + 1]].wait()
            push(at + 1)
        accumulate(at)
        if c:
            for i, q in units[k * share : (k + 1) * share]:
                consume(c - 1, i, q)
            if k == n_k - 1:
                write_sums(c - 1, part_a, (c - 1) * tiles_w)

    greetings = (n_cand - 1) + n_pts
    awaited = jnp.where(base, greetings - 1, greetings)
    awaited = awaited + jnp.where(speaks, pair * (n_cand - 1), 0)
    pl.semaphore_wait(barrier, awaited)
    send_parts(part_a, parts_a, a_send, a_recv)
    for i, q in units:
        consume(n_c - 1, i, q)
    write_sums(n_c - 1, part_b, 0)
    send_parts(part_b, parts_b, b_send, b_recv)

    for r in range(0, rows, PIECE):
        at = slice(r, r + PIECE)
        cover_of([last[at, t * LANES : (t + 1) * LANES] for t in range(tiles_w)], at, n_c - 1)
    for t in range(tiles_p):
        turned = jnp.transpose(b_acc[t * LANES : (t + 1) * LANES, :])
        best[t : t + 1, :] = jnp.max(turned, axis=0, keepdims=True)
    for k in range(1, n_cand):
        pltpu.make_async_remote_copy(
            src_ref=best, dst_ref=bests.at[mz], send_sem=best_send.at[0], recv_sem=best_recv.at[0],
            device_id={"cand": lax.rem(mz + k, n_cand)}, device_id_type=MESH,
        ).start()

    def settle(view, sem):
        pltpu.make_async_copy(view, view, sem).wait()

    def finish_cover():
        settle(bests.at[pl.ds(0, n_cand - 1)], best_recv.at[0])
        cover = best[...]
        for k in range(1, n_cand):
            cover = jnp.maximum(cover, bests[lax.rem(mz + k, n_cand)])
        cover_out[...] = jnp.maximum(v_buf[...], cover * scale)
        settle(bests.at[pl.ds(0, n_cand - 1)], best_send.at[0])

    place = lax.broadcasted_iota(jnp.int32, (8, LANES), 1).astype(F32)
    lane = lax.broadcasted_iota(jnp.int32, (1, LANES), 1)

    def merge(new):
        for i, row in enumerate(new):
            n_col[i * LANES : (i + 1) * LANES, :] = column_tile(row)
        across = [jnp.broadcast_to(row, (8, LANES)) for row in new]
        across.append(jnp.broadcast_to(top_row[...], (8, LANES)))
        columns = [t_col[g * 8 : (g + 1) * 8, :] for g in range(TOPK // 8)]
        columns += [n_col[g * 8 : (g + 1) * 8, :] for g in range(len(new) * LANES // 8)]
        kept = jnp.full((8, LANES), HIGH, F32)
        for column in columns:
            above = jnp.zeros((8, LANES), F32)
            for row in across:
                above = above + jnp.where(row > column, 1.0, 0.0)
            above = jnp.sum(above, axis=1, keepdims=True)
            kept = jnp.minimum(kept, jnp.where(above <= place, column, HIGH))
        kept = jnp.min(kept, axis=0, keepdims=True)
        return jnp.where(lane < TOPK, kept, LOW)

    def told(z, k, src, dst, send, recv):
        return pltpu.make_async_remote_copy(
            src_ref=src, dst_ref=dst, send_sem=send.at[0], recv_sem=recv.at[0],
            device_id={"pts": me - pair + 1 + k, "cand": z}, device_id_type=MESH,
        )

    @pl.when(base)
    def _():
        top_row[...] = jnp.where(lane < TOPK, -1.0, LOW)
        for z in range(n_cand):
            count = n_pts - 1 if z == 0 else n_pts
            for slots, recv, first, many in (
                (parts_a, a_recv, 0, rows_a), (parts_b, b_recv, rows_a, rows_b)
            ):
                t_col[...] = column_tile(top_row[...])[:TOPK, :]
                settle(slots.at[0, pl.ds(0, count)], recv.at[z])
                total = slots[z, 0]
                for p in range(1, n_pts):
                    total = total + slots[z, p]
                all_gains[z, first : first + many, :] = total
                top_row[...] = merge([total[t : t + 1, :] for t in range(many)])
            if z:
                @pl.when(speaks)
                def _():
                    for k in range(pair):
                        told(z, k, all_gains.at[z], got_gains, gain_send, gain_recv).start()
            if z == n_cand - 2:
                finish_cover()
                gains_out[...] = all_gains[0]
                settle(parts_a.at[0, pl.ds(0, n_pts - 1)], a_send.at[0])
                settle(parts_b.at[0, pl.ds(0, n_pts - 1)], b_send.at[0])
        top_out[...] = top_row[:, :TOPK]

        @pl.when(speaks)
        def _():
            for z in range(1, n_cand):
                for k in range(pair):
                    told(z, k, top_row, got_top, top_send, top_recv).start()
            many = pair * (n_cand - 1)
            for k in range(many):
                settle(got_gains, gain_send.at[0])
                settle(got_top, top_send.at[0])

    @pl.when(jnp.logical_not(base))
    def _():
        finish_cover()
        settle(parts_a.at[0, pl.ds(0, n_pts)], a_send.at[0])
        settle(parts_b.at[0, pl.ds(0, n_pts)], b_send.at[0])
        settle(got_gains, gain_recv.at[0])
        gains_out[...] = got_gains[...]
        settle(got_top, top_recv.at[0])
        top_out[...] = got_top[:, :TOPK]


def finish(gains, top, cover, gains_out, top_out, cover_out, sems):
    copies = [
        pltpu.make_async_copy(top, top_out, sems.at[0]),
        pltpu.make_async_copy(gains, gains_out, sems.at[1]),
        pltpu.make_async_copy(cover, cover_out, sems.at[2]),
    ]
    for copy in copies:
        copy.start()
    for copy in copies:
        copy.wait()


def solution(mesh):
    n_pts, n_cand = mesh.shape["pts"], mesh.shape["cand"]

    def on_device(points, weights, coverage, candidates, picks):
        rows, depth = points.shape
        cands = candidates.shape[0]
        tp, tc = rows // LANES, cands // LANES
        tb = WIDE // LANES
        ta = tc - tb
        anywhere = pl.BlockSpec(memory_space=pl.ANY)
        dma = pltpu.SemaphoreType.DMA
        vmem = pltpu.VMEM

        def scoped(*refs):
            many = rows // 2 // PIECE
            accs = [pltpu.ACC(q)((PIECE, WIDE), F32) for q in (0,) * many + (1,) * many] * 2
            pl.run_scoped(functools.partial(kernel, n_pts, n_cand, *refs), *accs)

        gains, top, cover = pl.pallas_call(
            scoped,
            out_shape=(vmem((tc, LANES), F32), vmem((1, TOPK), F32), vmem((tp, LANES), F32)),
            in_specs=[anywhere] * 5,
            out_specs=(pl.BlockSpec(memory_space=vmem),) * 3,
            scratch_shapes=[
                vmem((rows, depth), points.dtype), vmem((cands, depth), candidates.dtype),
                vmem((tp, LANES), F32), vmem((tp, LANES), F32),
                pltpu.SMEM(picks.shape, jnp.int32),
                vmem((rows, LANES), F32), vmem((rows, LANES), F32), vmem((rows, LANES), F32),
                vmem((rows, WIDE), F32),
                vmem((ta, LANES), F32), vmem((tb, LANES), F32),
                vmem((n_cand, n_pts, ta, LANES), F32), vmem((n_cand, n_pts, tb, LANES), F32),
                vmem((tp, LANES), F32), vmem((n_cand, tp, LANES), F32),
                vmem((n_cand, tc, LANES), F32), vmem((cands, LANES), F32), vmem((TOPK, LANES), F32),
                vmem((1, LANES), F32), vmem((tc, LANES), F32), vmem((1, LANES), F32),
                dma(((depth // WIDE) * (cands // WIDE + 1),)), dma((3,)),
                dma((1,)), dma((n_cand,)), dma((1,)), dma((n_cand,)), dma((1,)), dma((1,)),
                dma((1,)), dma((1,)), dma((1,)), dma((1,)),
            ],
            compiler_params=pltpu.CompilerParams(
                collective_id=0, has_side_effects=True, vmem_limit_bytes=60 * 2**20
            ),
            name="facility",
        )(points, weights.reshape(tp, LANES), coverage.reshape(tp, LANES), candidates, picks)
        gains, top, cover = pl.pallas_call(
            finish,
            out_shape=(
                jax.ShapeDtypeStruct((tc, LANES), F32),
                jax.ShapeDtypeStruct((1, TOPK), F32),
                jax.ShapeDtypeStruct((tp, LANES), F32),
            ),
            in_specs=[pl.BlockSpec(memory_space=vmem)] * 3,
            out_specs=(anywhere,) * 3,
            scratch_shapes=[dma((3,))],
            name="finish",
        )(*(pltpu.with_memory_space_constraint(x, vmem) for x in (gains, top, cover)))
        return gains.reshape(cands), top.reshape(TOPK), cover.reshape(rows)

    placed = (P("pts", None), P("pts"), P("pts"), P("cand", None), P())
    return jax.shard_map(
        on_device, mesh=mesh, in_specs=placed, out_specs=(P("cand"), P(), P("pts")), check_vma=False
    )
```

```python
import functools

import jax
import jax.numpy as jnp
from jax import lax
from jax.experimental import pallas as pl
from jax.experimental.pallas import tpu as pltpu
from jax.sharding import PartitionSpec as P

TOPK = 64
LANES = 128
MESH = pl.DeviceIdType.MESH
F32 = jnp.float32
LOW = -1e30
HIGH = 3e38
WIDE = 256
PIECE = 64


def column_tile(row):
    return jnp.transpose(jnp.broadcast_to(row, (LANES, LANES)))


def kernel(
    n_pts, n_cand, points, weights, coverage, candidates, picks, gains_out, top_out, cover_out,
    p_buf, c_buf, w_buf, v_buf, k_buf, w_col, v_col, b_acc, last, part_a, part_b, parts_a, parts_b,
    best, bests, all_gains, n_col, t_col, top_row, got_gains, got_top,
    in_sem, small_sem, a_send, a_recv, b_send, b_recv, best_send, best_recv,
    gain_send, gain_recv, top_send, top_recv, sent, heard, *accs,
):
    rows, depth = points.shape
    cands = candidates.shape[0]
    me, mz = lax.axis_index("pts"), lax.axis_index("cand")
    n_k, n_c = depth // WIDE, cands // WIDE
    half = rows // 2
    pieces = half // PIECE
    tiles_p, tiles_c = rows // LANES, cands // LANES
    tiles_w = WIDE // LANES
    rows_b = tiles_w
    rows_a = tiles_c - rows_b
    pair = 2 if n_pts % 2 == 0 else 1
    scale = depth ** (-0.5)

    steps = [(c, k) for c in range(n_c) for k in range(n_k)]
    spans = [("c", 0, 1)] + [("p", k, k + 1) for k in range(n_k)] + [("c", 1, 2), ("c", 2, n_c)]
    spans = [span for span in spans if span[1] < span[2]]
    loads = {}
    for at, (kind, first, after) in enumerate(spans):
        span = pl.ds(first * WIDE, (after - first) * WIDE)
        if kind == "p":
            src, dst = points.at[:, span], p_buf.at[:, span]
        else:
            src, dst = candidates.at[span, :], c_buf.at[span, :]
        loads[kind, first] = pltpu.make_async_copy(src, dst, in_sem.at[at])
    small = [
        pltpu.make_async_copy(weights, w_buf, small_sem.at[0]),
        pltpu.make_async_copy(coverage, v_buf, small_sem.at[1]),
        pltpu.make_async_copy(picks, k_buf, small_sem.at[2]),
    ]
    for copy in small:
        copy.start()
    for copy in loads.values():
        copy.start()

    base = mz == 0
    relay = me // pair * pair + pair - 1
    speaks = base & (me == relay)
    calls = base & (me == n_pts - 1)
    barrier = pltpu.get_barrier_semaphore()

    def greet(p, z):
        pl.semaphore_signal(barrier, inc=1, device_id={"pts": p, "cand": z}, device_id_type=MESH)

    @pl.when(base)
    def _():
        for z in range(n_cand):
            for k in range(n_pts):
                if z == 0 and k == 0:
                    continue
                greet(lax.rem(me + k, n_pts), z)

    for k in range(1, n_cand):
        greet(me, lax.rem(mz + k, n_cand))

    @pl.when(jnp.logical_not(base))
    def _():
        greet(relay, 0)
        greet(n_pts - 1, 0)

    for copy in small:
        copy.wait()
    w_row = w_buf[...] * (scale / (rows * n_pts))
    v_row = v_buf[...] * (1.0 / scale)
    for t in range(tiles_p):
        w_col[t * LANES : (t + 1) * LANES, :] = column_tile(w_row[t : t + 1, :])
        v_col[t * LANES : (t + 1) * LANES, :] = column_tile(v_row[t : t + 1, :])
    column = mz * cands + lax.broadcasted_iota(jnp.int32, (tiles_c, LANES), 0) * LANES
    column = column + lax.broadcasted_iota(jnp.int32, (tiles_c, LANES), 1)
    chosen = jnp.zeros((tiles_c, LANES), jnp.bool_)
    for k in range(picks.shape[0]):
        chosen = chosen | (column == k_buf[k])
    penalty = jnp.where(chosen, 0.0, LOW)

    def push(at):
        c, k = steps[at]
        tile = c_buf[c * WIDE : (c + 1) * WIDE, k * WIDE : (k + 1) * WIDE]
        for q in range(2):
            pltpu.matmul_push_rhs(tile, staging_register=at % 2, mxu_index=q, transpose=True)

    def accumulator(c, i, q):
        return accs[((c % 2) * 2 + q) * pieces + i]

    def accumulate(at):
        c, k = steps[at]
        for i in range(pieces):
            for q in range(2):
                from_p = q * half + i * PIECE
                pltpu.matmul_acc_lhs(
                    accumulator(c, i, q),
                    p_buf[from_p : from_p + PIECE, k * WIDE : (k + 1) * WIDE],
                    load_staged_rhs=at % 2 if i == 0 else None,
                )

    sums = {}

    def gain_of(x, at, c, t):
        value = jnp.maximum(x - v_col[at, :], 0.0) * w_col[at, :]
        value = jnp.sum(value.reshape(PIECE // 8, 8, LANES), axis=0)
        sums[c, t] = sums[c, t] + value if (c, t) in sums else value

    def cover_of(xs, at, c):
        found = b_acc[at, :] if c else None
        for t, x in enumerate(xs):
            tile = c * tiles_w + t
            x = x + penalty[tile : tile + 1, :]
            found = x if found is None else jnp.maximum(found, x)
        b_acc[at, :] = found

    def consume(c, i, q):
        from_p = q * half + i * PIECE
        at = slice(from_p, from_p + PIECE)
        sims = pltpu.matmul_pop(accumulator(c, i, q))
        xs = [sims[:, t * LANES : (t + 1) * LANES] for t in range(tiles_w)]
        for t, x in enumerate(xs):
            gain_of(x, at, c, t)
        if c + 1 < n_c:
            cover_of(xs, at, c)
        else:
            last[at, :] = sims

    def write_sums(c, dst, row):
        for t in range(tiles_w):
            dst[row + t : row + t + 1, :] = jnp.sum(sums[c, t], axis=0, keepdims=True)

    def send_parts(src, slots, send, recv):
        slots[0, me] = src[...]
        for k in range(n_pts):
            p = k + jnp.where(base & (k >= me), 1, 0)
            copy = pltpu.make_async_remote_copy(
                src_ref=src, dst_ref=slots.at[mz, me], send_sem=send.at[0], recv_sem=recv.at[mz],
                device_id={"pts": p, "cand": 0}, device_id_type=MESH,
            )
            if k + 1 < n_pts:
                copy.start()
            else:
                pl.when(jnp.logical_not(base))(copy.start)

    loads["c", 0].wait()
    push(0)
    units = [(i, q) for i in range(pieces) for q in range(2)]
    share = len(units) // n_k
    for at, (c, k) in enumerate(steps):
        if c == 0:
            loads["p", k].wait()
        if at + 1 < len(steps):
            if k + 1 == n_k and ("c", c + 1) in loads:
                loads["c", c + 1].wait()
            push(at + 1)
        accumulate(at)
        if c:
            for i, q in units[k * share : (k + 1) * share]:
                consume(c - 1, i, q)
            if k == n_k - 1:
                write_sums(c - 1, part_a, (c - 1) * tiles_w)

    greetings = (n_cand - 1) + n_pts
    awaited = jnp.where(base, greetings - 1, greetings)
    awaited = awaited + jnp.where(speaks, pair * (n_cand - 1), 0)
    awaited = awaited + jnp.where(calls, n_pts * (n_cand - 1), 0)
    pl.semaphore_wait(barrier, awaited)
    send_parts(part_a, parts_a, a_send, a_recv)
    for i, q in units:
        consume(n_c - 1, i, q)
    write_sums(n_c - 1, part_b, 0)
    send_parts(part_b, parts_b, b_send, b_recv)

    for r in range(0, rows, PIECE):
        at = slice(r, r + PIECE)
        cover_of([last[at, t * LANES : (t + 1) * LANES] for t in range(tiles_w)], at, n_c - 1)
    for t in range(tiles_p):
        turned = jnp.transpose(b_acc[t * LANES : (t + 1) * LANES, :])
        best[t : t + 1, :] = jnp.max(turned, axis=0, keepdims=True)
    for k in range(1, n_cand):
        pltpu.make_async_remote_copy(
            src_ref=best, dst_ref=bests.at[mz], send_sem=best_send.at[0], recv_sem=best_recv.at[0],
            device_id={"cand": lax.rem(mz + k, n_cand)}, device_id_type=MESH,
        ).start()

    def settle(view, sem):
        pltpu.make_async_copy(view, view, sem).wait()

    def finish_cover():
        settle(bests.at[pl.ds(0, n_cand - 1)], best_recv.at[0])
        cover = best[...]
        for k in range(1, n_cand):
            cover = jnp.maximum(cover, bests[lax.rem(mz + k, n_cand)])
        cover_out[...] = jnp.maximum(v_buf[...], cover * scale)
        settle(bests.at[pl.ds(0, n_cand - 1)], best_send.at[0])

    place = lax.broadcasted_iota(jnp.int32, (8, LANES), 1).astype(F32)
    lane = lax.broadcasted_iota(jnp.int32, (1, LANES), 1)

    def merge(new):
        for i, row in enumerate(new):
            n_col[i * LANES : (i + 1) * LANES, :] = column_tile(row)
        across = [jnp.broadcast_to(row, (8, LANES)) for row in new]
        across.append(jnp.broadcast_to(top_row[...], (8, LANES)))
        columns = [t_col[g * 8 : (g + 1) * 8, :] for g in range(TOPK // 8)]
        columns += [n_col[g * 8 : (g + 1) * 8, :] for g in range(len(new) * LANES // 8)]
        kept = jnp.full((8, LANES), HIGH, F32)
        for column in columns:
            above = jnp.zeros((8, LANES), F32)
            for row in across:
                above = above + jnp.where(row > column, 1.0, 0.0)
            above = jnp.sum(above, axis=1, keepdims=True)
            kept = jnp.minimum(kept, jnp.where(above <= place, column, HIGH))
        kept = jnp.min(kept, axis=0, keepdims=True)
        return jnp.where(lane < TOPK, kept, LOW)

    def told(p, z, src, dst, send, recv):
        return pltpu.make_async_remote_copy(
            src_ref=src, dst_ref=dst, send_sem=send.at[0], recv_sem=recv.at[0],
            device_id={"pts": p, "cand": z}, device_id_type=MESH,
        )

    @pl.when(base)
    def _():
        top_row[...] = jnp.where(lane < TOPK, -1.0, LOW)
        for z in range(n_cand):
            count = n_pts - 1 if z == 0 else n_pts
            for slots, recv, first, many in (
                (parts_a, a_recv, 0, rows_a), (parts_b, b_recv, rows_a, rows_b)
            ):
                t_col[...] = column_tile(top_row[...])[:TOPK, :]
                settle(slots.at[0, pl.ds(0, count)], recv.at[z])
                total = slots[z, 0]
                for p in range(1, n_pts):
                    total = total + slots[z, p]
                all_gains[z, first : first + many, :] = total
                top_row[...] = merge([total[t : t + 1, :] for t in range(many)])
            if z:
                @pl.when(speaks)
                def _():
                    for k in range(pair):
                        told(relay - k, z, all_gains.at[z], got_gains, gain_send, gain_recv).start()
            if z == n_cand - 2:
                finish_cover()
                gains_out[...] = all_gains[0]
                settle(parts_a.at[0, pl.ds(0, n_pts - 1)], a_send.at[0])
                settle(parts_b.at[0, pl.ds(0, n_pts - 1)], b_send.at[0])
        top_out[...] = top_row[:, :TOPK]

        @pl.when(calls)
        def _():
            for z in range(1, n_cand):
                for p in range(n_pts):
                    told(p, z, top_row, got_top, top_send, top_recv).start()

        @pl.when(speaks)
        def _():
            settle(sent.at[pl.ds(0, pair * (n_cand - 1))], gain_send.at[0])

        @pl.when(calls)
        def _():
            settle(heard, top_send.at[0])

    @pl.when(jnp.logical_not(base))
    def _():
        finish_cover()
        settle(parts_a.at[0, pl.ds(0, n_pts)], a_send.at[0])
        settle(parts_b.at[0, pl.ds(0, n_pts)], b_send.at[0])
        settle(got_gains, gain_recv.at[0])
        gains_out[...] = got_gains[...]
        settle(got_top, top_recv.at[0])
        top_out[...] = got_top[:, :TOPK]


def finish(gains, top, cover, gains_out, top_out, cover_out, sems):
    copies = [
        pltpu.make_async_copy(top, top_out, sems.at[0]),
        pltpu.make_async_copy(gains, gains_out, sems.at[1]),
        pltpu.make_async_copy(cover, cover_out, sems.at[2]),
    ]
    for copy in copies:
        copy.start()
    for copy in copies:
        copy.wait()


def solution(mesh):
    n_pts, n_cand = mesh.shape["pts"], mesh.shape["cand"]

    def on_device(points, weights, coverage, candidates, picks):
        rows, depth = points.shape
        cands = candidates.shape[0]
        tp, tc = rows // LANES, cands // LANES
        tb = WIDE // LANES
        ta = tc - tb
        anywhere = pl.BlockSpec(memory_space=pl.ANY)
        dma = pltpu.SemaphoreType.DMA
        vmem = pltpu.VMEM

        def scoped(*refs):
            many = rows // 2 // PIECE
            accs = [pltpu.ACC(q)((PIECE, WIDE), F32) for q in (0,) * many + (1,) * many] * 2
            pl.run_scoped(functools.partial(kernel, n_pts, n_cand, *refs), *accs)

        gains, top, cover = pl.pallas_call(
            scoped,
            out_shape=(vmem((tc, LANES), F32), vmem((1, TOPK), F32), vmem((tp, LANES), F32)),
            in_specs=[anywhere] * 5,
            out_specs=(pl.BlockSpec(memory_space=vmem),) * 3,
            scratch_shapes=[
                vmem((rows, depth), points.dtype), vmem((cands, depth), candidates.dtype),
                vmem((tp, LANES), F32), vmem((tp, LANES), F32),
                pltpu.SMEM(picks.shape, jnp.int32),
                vmem((rows, LANES), F32), vmem((rows, LANES), F32), vmem((rows, LANES), F32),
                vmem((rows, WIDE), F32),
                vmem((ta, LANES), F32), vmem((tb, LANES), F32),
                vmem((n_cand, n_pts, ta, LANES), F32), vmem((n_cand, n_pts, tb, LANES), F32),
                vmem((tp, LANES), F32), vmem((n_cand, tp, LANES), F32),
                vmem((n_cand, tc, LANES), F32), vmem((cands, LANES), F32), vmem((TOPK, LANES), F32),
                vmem((1, LANES), F32), vmem((tc, LANES), F32), vmem((1, LANES), F32),
                dma((depth // WIDE + 3,)), dma((3,)),
                dma((1,)), dma((n_cand,)), dma((1,)), dma((n_cand,)), dma((1,)), dma((1,)),
                dma((1,)), dma((1,)), dma((1,)), dma((1,)),
                vmem((2 * (n_cand - 1), tc, LANES), F32), vmem((n_pts * (n_cand - 1), 1, LANES), F32),
            ],
            compiler_params=pltpu.CompilerParams(
                collective_id=0, has_side_effects=True, vmem_limit_bytes=60 * 2**20,
            ),
            name="facility",
        )(points, weights.reshape(tp, LANES), coverage.reshape(tp, LANES), candidates, picks)
        gains, top, cover = pl.pallas_call(
            finish,
            out_shape=(
                jax.ShapeDtypeStruct((tc, LANES), F32),
                jax.ShapeDtypeStruct((1, TOPK), F32),
                jax.ShapeDtypeStruct((tp, LANES), F32),
            ),
            in_specs=[pl.BlockSpec(memory_space=vmem)] * 3,
            out_specs=(anywhere,) * 3,
            scratch_shapes=[dma((3,))],
            name="finish",
        )(*(pltpu.with_memory_space_constraint(x, vmem) for x in (gains, top, cover)))
        return gains.reshape(cands), top.reshape(TOPK), cover.reshape(rows)

    placed = (P("pts", None), P("pts"), P("pts"), P("cand", None), P())
    return jax.shard_map(
        on_device, mesh=mesh, in_specs=placed, out_specs=(P("cand"), P(), P("pts")), check_vma=False
    )
```

```python
import functools

import jax
import jax.numpy as jnp
from jax import lax
from jax.experimental import pallas as pl
from jax.experimental.pallas import tpu as pltpu
from jax.sharding import PartitionSpec as P

TOPK = 64
LANES = 128
MESH = pl.DeviceIdType.MESH
F32 = jnp.float32
LOW = -1e30
HIGH = 3e38
WIDE = 256
PIECE = 64


def column_tile(row):
    return jnp.transpose(jnp.broadcast_to(row, (LANES, LANES)))


def kernel(
    n_pts, n_cand, points, weights, coverage, candidates, picks, gains_out, top_out, cover_out,
    p_buf, c_buf, w_buf, v_buf, k_buf, w_col, v_col, b_acc, last, part_a, part_b, parts_a, parts_b,
    best, bests, all_gains, n_col, t_col, top_row, got_gains, got_top,
    in_sem, small_sem, a_send, a_recv, b_send, b_recv, best_send, best_recv,
    gain_send, gain_recv, top_send, top_recv, sent_a, sent_b, sent, heard, *accs,
):
    rows, depth = points.shape
    cands = candidates.shape[0]
    me, mz = lax.axis_index("pts"), lax.axis_index("cand")
    n_k, n_c = depth // WIDE, cands // WIDE
    half = rows // 2
    pieces = half // PIECE
    tiles_p, tiles_c = rows // LANES, cands // LANES
    tiles_w = WIDE // LANES
    rows_b = tiles_w
    rows_a = tiles_c - rows_b
    scale = depth ** (-0.5)

    steps = [(c, k) for c in range(n_c) for k in range(n_k)]
    spans = [("c", 0, 1)] + [("p", k, k + 1) for k in range(n_k)] + [("c", 1, 2), ("c", 2, n_c)]
    spans = [span for span in spans if span[1] < span[2]]
    loads = {}
    for at, (kind, first, after) in enumerate(spans):
        span = pl.ds(first * WIDE, (after - first) * WIDE)
        if kind == "p":
            src, dst = points.at[:, span], p_buf.at[:, span]
        else:
            src, dst = candidates.at[span, :], c_buf.at[span, :]
        loads[kind, first] = pltpu.make_async_copy(src, dst, in_sem.at[at])
    small = [
        pltpu.make_async_copy(weights, w_buf, small_sem.at[0]),
        pltpu.make_async_copy(coverage, v_buf, small_sem.at[1]),
        pltpu.make_async_copy(picks, k_buf, small_sem.at[2]),
    ]
    for copy in small:
        copy.start()
    for copy in loads.values():
        copy.start()

    base = mz == 0
    final = me == n_pts - 1
    ranks = base | final
    calls = final & jnp.logical_not(base)
    barrier = pltpu.get_barrier_semaphore()

    def greet(p, z):
        pl.semaphore_signal(barrier, inc=1, device_id={"pts": p, "cand": z}, device_id_type=MESH)

    @pl.when(ranks)
    def _():
        for z in range(n_cand):
            for k in range(n_pts):
                if z == 0 and k == 0:
                    continue
                greet(lax.rem(me + k, n_pts), lax.rem(mz + z, n_cand))

    for k in range(1, n_cand):
        greet(me, lax.rem(mz + k, n_cand))

    @pl.when(jnp.logical_not(ranks))
    def _():
        greet(n_pts - 1, mz)

    for copy in small:
        copy.wait()
    w_row = w_buf[...] * (scale / (rows * n_pts))
    v_row = v_buf[...] * (1.0 / scale)
    for t in range(tiles_p):
        w_col[t * LANES : (t + 1) * LANES, :] = column_tile(w_row[t : t + 1, :])
        v_col[t * LANES : (t + 1) * LANES, :] = column_tile(v_row[t : t + 1, :])
    column = mz * cands + lax.broadcasted_iota(jnp.int32, (tiles_c, LANES), 0) * LANES
    column = column + lax.broadcasted_iota(jnp.int32, (tiles_c, LANES), 1)
    chosen = jnp.zeros((tiles_c, LANES), jnp.bool_)
    for k in range(picks.shape[0]):
        chosen = chosen | (column == k_buf[k])
    penalty = jnp.where(chosen, 0.0, LOW)

    def push(at):
        c, k = steps[at]
        tile = c_buf[c * WIDE : (c + 1) * WIDE, k * WIDE : (k + 1) * WIDE]
        for q in range(2):
            pltpu.matmul_push_rhs(tile, staging_register=at % 2, mxu_index=q, transpose=True)

    def accumulator(c, i, q):
        return accs[((c % 2) * 2 + q) * pieces + i]

    def accumulate(at):
        c, k = steps[at]
        for i in range(pieces):
            for q in range(2):
                from_p = q * half + i * PIECE
                pltpu.matmul_acc_lhs(
                    accumulator(c, i, q),
                    p_buf[from_p : from_p + PIECE, k * WIDE : (k + 1) * WIDE],
                    load_staged_rhs=at % 2 if i == 0 else None,
                )

    sums = {}

    def gain_of(x, at, c, t):
        value = jnp.maximum(x - v_col[at, :], 0.0) * w_col[at, :]
        value = jnp.sum(value.reshape(PIECE // 8, 8, LANES), axis=0)
        sums[c, t] = sums[c, t] + value if (c, t) in sums else value

    def cover_of(xs, at, c):
        found = b_acc[at, :] if c else None
        for t, x in enumerate(xs):
            tile = c * tiles_w + t
            x = x + penalty[tile : tile + 1, :]
            found = x if found is None else jnp.maximum(found, x)
        b_acc[at, :] = found

    def consume(c, i, q):
        from_p = q * half + i * PIECE
        at = slice(from_p, from_p + PIECE)
        sims = pltpu.matmul_pop(accumulator(c, i, q))
        xs = [sims[:, t * LANES : (t + 1) * LANES] for t in range(tiles_w)]
        for t, x in enumerate(xs):
            gain_of(x, at, c, t)
        if c + 1 < n_c:
            cover_of(xs, at, c)
        else:
            last[at, :] = sims

    def write_sums(c, dst, row):
        for t in range(tiles_w):
            dst[row + t : row + t + 1, :] = jnp.sum(sums[c, t], axis=0, keepdims=True)

    def send_parts(src, slots, send, recv):
        def to(p, z):
            return pltpu.make_async_remote_copy(
                src_ref=src, dst_ref=slots.at[mz, me], send_sem=send.at[0], recv_sem=recv.at[mz],
                device_id={"pts": p, "cand": z}, device_id_type=MESH,
            )

        slots[mz, me] = src[...]
        for k in range(n_pts - 1):
            to(k + jnp.where(base & (k >= me), 1, 0), 0).start()
        pl.when(jnp.logical_not(base))(to(n_pts - 1, 0).start)
        for z in range(1, n_cand):
            pl.when(jnp.logical_not(final & (mz == z)))(to(n_pts - 1, z).start)

    loads["c", 0].wait()
    push(0)
    units = [(i, q) for i in range(pieces) for q in range(2)]
    share = len(units) // n_k
    for at, (c, k) in enumerate(steps):
        if c == 0:
            loads["p", k].wait()
        if at + 1 < len(steps):
            if k + 1 == n_k and ("c", c + 1) in loads:
                loads["c", c + 1].wait()
            push(at + 1)
        accumulate(at)
        if c:
            for i, q in units[k * share : (k + 1) * share]:
                consume(c - 1, i, q)
            if k == n_k - 1:
                write_sums(c - 1, part_a, (c - 1) * tiles_w)

    rankers = n_pts + n_cand - 1
    awaited = (n_cand - 1) + rankers - jnp.where(ranks, 1, 0) + jnp.where(calls, n_pts - 1, 0)
    pl.semaphore_wait(barrier, awaited)
    send_parts(part_a, parts_a, a_send, a_recv)
    for i, q in units:
        consume(n_c - 1, i, q)
    write_sums(n_c - 1, part_b, 0)
    send_parts(part_b, parts_b, b_send, b_recv)

    for r in range(0, rows, PIECE):
        at = slice(r, r + PIECE)
        cover_of([last[at, t * LANES : (t + 1) * LANES] for t in range(tiles_w)], at, n_c - 1)
    for t in range(tiles_p):
        turned = jnp.transpose(b_acc[t * LANES : (t + 1) * LANES, :])
        best[t : t + 1, :] = jnp.max(turned, axis=0, keepdims=True)
    for k in range(1, n_cand):
        pltpu.make_async_remote_copy(
            src_ref=best, dst_ref=bests.at[mz], send_sem=best_send.at[0], recv_sem=best_recv.at[0],
            device_id={"cand": lax.rem(mz + k, n_cand)}, device_id_type=MESH,
        ).start()

    def settle(view, sem):
        pltpu.make_async_copy(view, view, sem).wait()

    def finish_cover():
        settle(bests.at[pl.ds(0, n_cand - 1)], best_recv.at[0])
        cover = best[...]
        for k in range(1, n_cand):
            cover = jnp.maximum(cover, bests[lax.rem(mz + k, n_cand)])
        cover_out[...] = jnp.maximum(v_buf[...], cover * scale)
        settle(bests.at[pl.ds(0, n_cand - 1)], best_send.at[0])

    place = lax.broadcasted_iota(jnp.int32, (8, LANES), 1).astype(F32)
    lane = lax.broadcasted_iota(jnp.int32, (1, LANES), 1)

    def merge(new):
        for i, row in enumerate(new):
            n_col[i * LANES : (i + 1) * LANES, :] = column_tile(row)
        across = [jnp.broadcast_to(row, (8, LANES)) for row in new]
        across.append(jnp.broadcast_to(top_row[...], (8, LANES)))
        columns = [t_col[g * 8 : (g + 1) * 8, :] for g in range(TOPK // 8)]
        columns += [n_col[g * 8 : (g + 1) * 8, :] for g in range(len(new) * LANES // 8)]
        kept = jnp.full((8, LANES), HIGH, F32)
        for column in columns:
            above = jnp.zeros((8, LANES), F32)
            for row in across:
                above = above + jnp.where(row > column, 1.0, 0.0)
            above = jnp.sum(above, axis=1, keepdims=True)
            kept = jnp.minimum(kept, jnp.where(above <= place, column, HIGH))
        kept = jnp.min(kept, axis=0, keepdims=True)
        return jnp.where(lane < TOPK, kept, LOW)

    def told(p, src, dst, send, recv):
        return pltpu.make_async_remote_copy(
            src_ref=src, dst_ref=dst, send_sem=send.at[0], recv_sem=recv.at[0],
            device_id={"pts": p}, device_id_type=MESH,
        )

    def settle_either(fewer, view, many, sem):
        pl.when(fewer)(lambda: settle(view.at[pl.ds(0, many - 1)], sem))
        pl.when(jnp.logical_not(fewer))(lambda: settle(view.at[pl.ds(0, many)], sem))

    def settle_sends():
        settle_either(ranks, sent_a, rankers, a_send.at[0])
        settle_either(ranks, sent_b, rankers, b_send.at[0])

    @pl.when(ranks)
    def _():
        top_row[...] = jnp.where(lane < TOPK, -1.0, LOW)
        for z in range(n_cand):
            for slots, recv, first, many in (
                (parts_a, a_recv, 0, rows_a), (parts_b, b_recv, rows_a, rows_b)
            ):
                t_col[...] = column_tile(top_row[...])[:TOPK, :]
                settle_either(mz == z, slots.at[0], n_pts, recv.at[z])
                total = slots[z, 0]
                for p in range(1, n_pts):
                    total = total + slots[z, p]
                all_gains[z, first : first + many, :] = total
                top_row[...] = merge([total[t : t + 1, :] for t in range(many)])
            if z == max(n_cand - 2, 0):
                finish_cover()
                settle_sends()
        top_out[...] = top_row[:, :TOPK]
        gains_out[...] = all_gains[mz]

        @pl.when(calls)
        def _():
            for p in range(n_pts - 1):
                told(p, top_row, got_top, top_send, top_recv).start()
            for p in range(n_pts - 1):
                told(p, gains_out, got_gains, gain_send, gain_recv).start()
            settle(heard, top_send.at[0])
            settle(sent, gain_send.at[0])

    @pl.when(jnp.logical_not(ranks))
    def _():
        finish_cover()
        settle_sends()
        settle(got_gains, gain_recv.at[0])
        gains_out[...] = got_gains[...]
        settle(got_top, top_recv.at[0])
        top_out[...] = got_top[:, :TOPK]


def finish(gains, top, cover, gains_out, top_out, cover_out, sems):
    copies = [
        pltpu.make_async_copy(top, top_out, sems.at[0]),
        pltpu.make_async_copy(gains, gains_out, sems.at[1]),
        pltpu.make_async_copy(cover, cover_out, sems.at[2]),
    ]
    for copy in copies:
        copy.start()
    for copy in copies:
        copy.wait()


def solution(mesh):
    n_pts, n_cand = mesh.shape["pts"], mesh.shape["cand"]

    def on_device(points, weights, coverage, candidates, picks):
        rows, depth = points.shape
        cands = candidates.shape[0]
        tp, tc = rows // LANES, cands // LANES
        tb = WIDE // LANES
        ta = tc - tb
        anywhere = pl.BlockSpec(memory_space=pl.ANY)
        dma = pltpu.SemaphoreType.DMA
        vmem = pltpu.VMEM

        def scoped(*refs):
            many = rows // 2 // PIECE
            accs = [pltpu.ACC(q)((PIECE, WIDE), F32) for q in (0,) * many + (1,) * many] * 2
            pl.run_scoped(functools.partial(kernel, n_pts, n_cand, *refs), *accs)

        gains, top, cover = pl.pallas_call(
            scoped,
            out_shape=(vmem((tc, LANES), F32), vmem((1, TOPK), F32), vmem((tp, LANES), F32)),
            in_specs=[anywhere] * 5,
            out_specs=(pl.BlockSpec(memory_space=vmem),) * 3,
            scratch_shapes=[
                vmem((rows, depth), points.dtype), vmem((cands, depth), candidates.dtype),
                vmem((tp, LANES), F32), vmem((tp, LANES), F32),
                pltpu.SMEM(picks.shape, jnp.int32),
                vmem((rows, LANES), F32), vmem((rows, LANES), F32), vmem((rows, LANES), F32),
                vmem((rows, WIDE), F32),
                vmem((ta, LANES), F32), vmem((tb, LANES), F32),
                vmem((n_cand, n_pts, ta, LANES), F32), vmem((n_cand, n_pts, tb, LANES), F32),
                vmem((tp, LANES), F32), vmem((n_cand, tp, LANES), F32),
                vmem((n_cand, tc, LANES), F32), vmem((cands, LANES), F32), vmem((TOPK, LANES), F32),
                vmem((1, LANES), F32), vmem((tc, LANES), F32), vmem((1, LANES), F32),
                dma((depth // WIDE + 3,)), dma((3,)),
                dma((1,)), dma((n_cand,)), dma((1,)), dma((n_cand,)), dma((1,)), dma((1,)),
                dma((1,)), dma((1,)), dma((1,)), dma((1,)),
                vmem((n_pts + n_cand - 1, ta, LANES), F32), vmem((n_pts + n_cand - 1, tb, LANES), F32),
                vmem((n_pts - 1, tc, LANES), F32), vmem((n_pts - 1, 1, LANES), F32),
            ],
            compiler_params=pltpu.CompilerParams(
                collective_id=0, has_side_effects=True, vmem_limit_bytes=60 * 2**20,
            ),
            name="facility",
        )(points, weights.reshape(tp, LANES), coverage.reshape(tp, LANES), candidates, picks)
        gains, top, cover = pl.pallas_call(
            finish,
            out_shape=(
                jax.ShapeDtypeStruct((tc, LANES), F32),
                jax.ShapeDtypeStruct((1, TOPK), F32),
                jax.ShapeDtypeStruct((tp, LANES), F32),
            ),
            in_specs=[pl.BlockSpec(memory_space=vmem)] * 3,
            out_specs=(anywhere,) * 3,
            scratch_shapes=[dma((3,))],
            name="finish",
        )(*(pltpu.with_memory_space_constraint(x, vmem) for x in (gains, top, cover)))
        return gains.reshape(cands), top.reshape(TOPK), cover.reshape(rows)

    placed = (P("pts", None), P("pts"), P("pts"), P("cand", None), P())
    return jax.shard_map(
        on_device, mesh=mesh, in_specs=placed, out_specs=(P("cand"), P(), P("pts")), check_vma=False
    )
```

```python
import functools

import jax
import jax.numpy as jnp
from jax import lax
from jax.experimental import pallas as pl
from jax.experimental.pallas import tpu as pltpu
from jax.sharding import PartitionSpec as P

TOPK = 64
LANES = 128
MESH = pl.DeviceIdType.MESH
F32 = jnp.float32
LOW = -1e30
HIGH = 3e38
WIDE = 256
PIECE = 64


def column_tile(row):
    return jnp.transpose(jnp.broadcast_to(row, (LANES, LANES)))


def kernel(
    n_pts, n_cand, points, weights, coverage, candidates, picks, gains_out, top_out, cover_out,
    p_buf, c_buf, w_buf, v_buf, k_buf, w_col, v_col, b_acc, last, part_a, part_b, parts_a, parts_b,
    best, bests, all_gains, n_col, t_col, top_row, got_gains, got_top,
    in_sem, small_sem, a_send, a_recv, b_send, b_recv, best_send, best_recv,
    gain_send, gain_recv, top_send, top_recv, sent_a, sent_b, sent, heard, passed, *accs,
):
    rows, depth = points.shape
    cands = candidates.shape[0]
    me, mz = lax.axis_index("pts"), lax.axis_index("cand")
    n_k, n_c = depth // WIDE, cands // WIDE
    half = rows // 2
    pieces = half // PIECE
    tiles_p, tiles_c = rows // LANES, cands // LANES
    tiles_w = WIDE // LANES
    rows_b = tiles_w
    rows_a = tiles_c - rows_b
    scale = depth ** (-0.5)

    steps = [(c, k) for c in range(n_c) for k in range(n_k)]
    spans = [("c", 0, 1)] + [("p", k, k + 1) for k in range(n_k)] + [("c", 1, 2), ("c", 2, n_c)]
    spans = [span for span in spans if span[1] < span[2]]
    loads = {}
    for at, (kind, first, after) in enumerate(spans):
        span = pl.ds(first * WIDE, (after - first) * WIDE)
        if kind == "p":
            src, dst = points.at[:, span], p_buf.at[:, span]
        else:
            src, dst = candidates.at[span, :], c_buf.at[span, :]
        loads[kind, first] = pltpu.make_async_copy(src, dst, in_sem.at[at])
    small = [
        pltpu.make_async_copy(weights, w_buf, small_sem.at[0]),
        pltpu.make_async_copy(coverage, v_buf, small_sem.at[1]),
        pltpu.make_async_copy(picks, k_buf, small_sem.at[2]),
    ]
    for copy in small:
        copy.start()
    for copy in loads.values():
        copy.start()

    base = mz == 0
    final = me == n_pts - 1
    ranks = base | final
    calls = final & jnp.logical_not(base)
    barrier = pltpu.get_barrier_semaphore()

    def greet(p, z):
        pl.semaphore_signal(barrier, inc=1, device_id={"pts": p, "cand": z}, device_id_type=MESH)

    @pl.when(ranks)
    def _():
        for z in range(n_cand):
            for k in range(n_pts):
                if z == 0 and k == 0:
                    continue
                greet(lax.rem(me + k, n_pts), lax.rem(mz + z, n_cand))

    for k in range(1, n_cand):
        greet(me, lax.rem(mz + k, n_cand))

    @pl.when(jnp.logical_not(ranks))
    def _():
        greet(n_pts - 1, mz)

    for copy in small:
        copy.wait()
    w_row = w_buf[...] * (scale / (rows * n_pts))
    v_row = v_buf[...] * (1.0 / scale)
    for t in range(tiles_p):
        w_col[t * LANES : (t + 1) * LANES, :] = column_tile(w_row[t : t + 1, :])
        v_col[t * LANES : (t + 1) * LANES, :] = column_tile(v_row[t : t + 1, :])
    column = mz * cands + lax.broadcasted_iota(jnp.int32, (tiles_c, LANES), 0) * LANES
    column = column + lax.broadcasted_iota(jnp.int32, (tiles_c, LANES), 1)
    chosen = jnp.zeros((tiles_c, LANES), jnp.bool_)
    for k in range(picks.shape[0]):
        chosen = chosen | (column == k_buf[k])
    penalty = jnp.where(chosen, 0.0, LOW)

    def push(at):
        c, k = steps[at]
        tile = c_buf[c * WIDE : (c + 1) * WIDE, k * WIDE : (k + 1) * WIDE]
        for q in range(2):
            pltpu.matmul_push_rhs(tile, staging_register=at % 2, mxu_index=q, transpose=True)

    def accumulator(c, i, q):
        return accs[((c % 2) * 2 + q) * pieces + i]

    def accumulate(at):
        c, k = steps[at]
        for i in range(pieces):
            for q in range(2):
                from_p = q * half + i * PIECE
                pltpu.matmul_acc_lhs(
                    accumulator(c, i, q),
                    p_buf[from_p : from_p + PIECE, k * WIDE : (k + 1) * WIDE],
                    load_staged_rhs=at % 2 if i == 0 else None,
                )

    sums = {}

    def gain_of(x, at, c, t, lane):
        value = jnp.maximum(x - v_col[at, :], 0.0) * w_col[at, :]
        key = c, t, lane
        sums[key] = sums[key] + value if key in sums else value

    def cover_of(xs, at, c):
        found = b_acc[at, :] if c else None
        for t, x in enumerate(xs):
            tile = c * tiles_w + t
            x = x + penalty[tile : tile + 1, :]
            found = x if found is None else jnp.maximum(found, x)
        b_acc[at, :] = found

    def consume(c, i, q):
        from_p = q * half + i * PIECE
        sims = pltpu.matmul_pop(accumulator(c, i, q))
        for r in range(0, PIECE, 8):
            at = slice(from_p + r, from_p + r + 8)
            xs = [sims[r : r + 8, t * LANES : (t + 1) * LANES] for t in range(tiles_w)]
            for t, x in enumerate(xs):
                gain_of(x, at, c, t, q * 2 + r // 8 % 2)
            if c + 1 < n_c:
                cover_of(xs, at, c)
            else:
                last[at, :] = sims[r : r + 8, :]

    def write_sums(c, dst, row):
        for t in range(tiles_w):
            total = (sums[c, t, 0] + sums[c, t, 1]) + (sums[c, t, 2] + sums[c, t, 3])
            dst[row + t : row + t + 1, :] = jnp.sum(total, axis=0, keepdims=True)

    def send_parts(src, slots, send, recv):
        def to(p, z):
            return pltpu.make_async_remote_copy(
                src_ref=src, dst_ref=slots.at[mz, me], send_sem=send.at[0], recv_sem=recv.at[mz],
                device_id={"pts": p, "cand": z}, device_id_type=MESH,
            )

        for k in range(n_pts - 1):
            to(k + jnp.where(base & (k >= me), 1, 0), 0).start()
        pl.when(jnp.logical_not(base))(to(n_pts - 1, 0).start)
        for z in range(1, n_cand):
            pl.when(jnp.logical_not(final & (mz == z)))(to(n_pts - 1, z).start)
        slots[mz, me] = src[...]

    loads["c", 0].wait()
    push(0)
    units = [(i, q) for i in range(pieces) for q in range(2)]
    share = len(units) // n_k
    fences = []

    def fence():
        pl.semaphore_signal(passed, 1)
        fences.append(1)

    for at, (c, k) in enumerate(steps):
        if c and k % 2 == 0:
            fence()
        if c == 0:
            loads["p", k].wait()
        if at + 1 < len(steps):
            if k + 1 == n_k and ("c", c + 1) in loads:
                loads["c", c + 1].wait()
            push(at + 1)
        accumulate(at)
        if c:
            for i, q in units[k * share : (k + 1) * share]:
                consume(c - 1, i, q)
            if k == n_k - 1:
                write_sums(c - 1, part_a, (c - 1) * tiles_w)

    rankers = n_pts + n_cand - 1
    awaited = (n_cand - 1) + rankers - jnp.where(ranks, 1, 0) + jnp.where(calls, n_pts - 1, 0)
    pl.semaphore_wait(barrier, awaited)
    send_parts(part_a, parts_a, a_send, a_recv)
    for at, (i, q) in enumerate(units):
        if at and at % 2 == 0:
            fence()
        consume(n_c - 1, i, q)
    write_sums(n_c - 1, part_b, 0)
    send_parts(part_b, parts_b, b_send, b_recv)
    pl.semaphore_wait(passed, len(fences))

    for r in range(0, rows, PIECE):
        at = slice(r, r + PIECE)
        cover_of([last[at, t * LANES : (t + 1) * LANES] for t in range(tiles_w)], at, n_c - 1)
    for t in range(tiles_p):
        turned = jnp.transpose(b_acc[t * LANES : (t + 1) * LANES, :])
        best[t : t + 1, :] = jnp.max(turned, axis=0, keepdims=True)
    for k in range(1, n_cand):
        pltpu.make_async_remote_copy(
            src_ref=best, dst_ref=bests.at[mz], send_sem=best_send.at[0], recv_sem=best_recv.at[0],
            device_id={"cand": lax.rem(mz + k, n_cand)}, device_id_type=MESH,
        ).start()

    def settle(view, sem):
        pltpu.make_async_copy(view, view, sem).wait()

    def finish_cover():
        settle(bests.at[pl.ds(0, n_cand - 1)], best_recv.at[0])
        cover = best[...]
        for k in range(1, n_cand):
            cover = jnp.maximum(cover, bests[lax.rem(mz + k, n_cand)])
        cover_out[...] = jnp.maximum(v_buf[...], cover * scale)
        settle(bests.at[pl.ds(0, n_cand - 1)], best_send.at[0])

    place = lax.broadcasted_iota(jnp.int32, (8, LANES), 1).astype(F32)
    lane = lax.broadcasted_iota(jnp.int32, (1, LANES), 1)

    def merge(new):
        for i, row in enumerate(new):
            n_col[i * LANES : (i + 1) * LANES, :] = column_tile(row)
        across = [jnp.broadcast_to(row, (8, LANES)) for row in new]
        across.append(jnp.broadcast_to(top_row[...], (8, LANES)))
        columns = [t_col[g * 8 : (g + 1) * 8, :] for g in range(TOPK // 8)]
        columns += [n_col[g * 8 : (g + 1) * 8, :] for g in range(len(new) * LANES // 8)]
        kept = jnp.full((8, LANES), HIGH, F32)
        for column in columns:
            above = jnp.zeros((8, LANES), F32)
            for row in across:
                above = above + jnp.where(row > column, 1.0, 0.0)
            above = jnp.sum(above, axis=1, keepdims=True)
            kept = jnp.minimum(kept, jnp.where(above <= place, column, HIGH))
        kept = jnp.min(kept, axis=0, keepdims=True)
        return jnp.where(lane < TOPK, kept, LOW)

    def told(p, src, dst, send, recv):
        return pltpu.make_async_remote_copy(
            src_ref=src, dst_ref=dst, send_sem=send.at[0], recv_sem=recv.at[0],
            device_id={"pts": p}, device_id_type=MESH,
        )

    def settle_either(fewer, view, many, sem):
        pl.when(fewer)(lambda: settle(view.at[pl.ds(0, many - 1)], sem))
        pl.when(jnp.logical_not(fewer))(lambda: settle(view.at[pl.ds(0, many)], sem))

    def settle_sends():
        settle_either(ranks, sent_a, rankers, a_send.at[0])
        settle_either(ranks, sent_b, rankers, b_send.at[0])

    def send_gains(z):
        for p in range(n_pts - 1):
            told(p, all_gains.at[z], got_gains, gain_send, gain_recv).start()

    def tell_gains(z):
        if z:
            pl.when(final & (mz == z))(lambda: send_gains(z))

    @pl.when(ranks)
    def _():
        top_row[...] = jnp.where(lane < TOPK, -1.0, LOW)
        for z in range(n_cand):
            for slots, recv, first, many in (
                (parts_a, a_recv, 0, rows_a), (parts_b, b_recv, rows_a, rows_b)
            ):
                t_col[...] = column_tile(top_row[...])[:TOPK, :]
                settle_either(mz == z, slots.at[0], n_pts, recv.at[z])
                total = slots[z, 0]
                for p in range(1, n_pts):
                    total = total + slots[z, p]
                all_gains[z, first : first + many, :] = total
                if first and z + 1 < n_cand:
                    tell_gains(z)
                if first and z == max(n_cand - 2, 0):
                    finish_cover()
                    settle_sends()
                top_row[...] = merge([total[t : t + 1, :] for t in range(many)])
        top_out[...] = top_row[:, :TOPK]
        gains_out[...] = all_gains[mz]

        @pl.when(calls)
        def _():
            for p in range(n_pts - 1):
                told(p, top_row, got_top, top_send, top_recv).start()
            pl.when(mz == n_cand - 1)(lambda: send_gains(n_cand - 1))
            settle(heard, top_send.at[0])
            settle(sent, gain_send.at[0])

    @pl.when(jnp.logical_not(ranks))
    def _():
        finish_cover()
        settle_sends()
        settle(got_gains, gain_recv.at[0])
        gains_out[...] = got_gains[...]
        settle(got_top, top_recv.at[0])
        top_out[...] = got_top[:, :TOPK]


def finish(gains, top, cover, gains_out, top_out, cover_out, sems):
    copies = [
        pltpu.make_async_copy(top, top_out, sems.at[0]),
        pltpu.make_async_copy(gains, gains_out, sems.at[1]),
        pltpu.make_async_copy(cover, cover_out, sems.at[2]),
    ]
    for copy in copies:
        copy.start()
    for copy in copies:
        copy.wait()


def solution(mesh):
    n_pts, n_cand = mesh.shape["pts"], mesh.shape["cand"]

    def on_device(points, weights, coverage, candidates, picks):
        rows, depth = points.shape
        cands = candidates.shape[0]
        tp, tc = rows // LANES, cands // LANES
        tb = WIDE // LANES
        ta = tc - tb
        anywhere = pl.BlockSpec(memory_space=pl.ANY)
        dma = pltpu.SemaphoreType.DMA
        vmem = pltpu.VMEM

        def scoped(*refs):
            many = rows // 2 // PIECE
            accs = [pltpu.ACC(q)((PIECE, WIDE), F32) for q in (0,) * many + (1,) * many] * 2
            pl.run_scoped(functools.partial(kernel, n_pts, n_cand, *refs), *accs)

        gains, top, cover = pl.pallas_call(
            scoped,
            out_shape=(vmem((tc, LANES), F32), vmem((1, TOPK), F32), vmem((tp, LANES), F32)),
            in_specs=[anywhere] * 5,
            out_specs=(pl.BlockSpec(memory_space=vmem),) * 3,
            scratch_shapes=[
                vmem((rows, depth), points.dtype), vmem((cands, depth), candidates.dtype),
                vmem((tp, LANES), F32), vmem((tp, LANES), F32),
                pltpu.SMEM(picks.shape, jnp.int32),
                vmem((rows, LANES), F32), vmem((rows, LANES), F32), vmem((rows, LANES), F32),
                vmem((rows, WIDE), F32),
                vmem((ta, LANES), F32), vmem((tb, LANES), F32),
                vmem((n_cand, n_pts, ta, LANES), F32), vmem((n_cand, n_pts, tb, LANES), F32),
                vmem((tp, LANES), F32), vmem((n_cand, tp, LANES), F32),
                vmem((n_cand, tc, LANES), F32), vmem((cands, LANES), F32), vmem((TOPK, LANES), F32),
                vmem((1, LANES), F32), vmem((tc, LANES), F32), vmem((1, LANES), F32),
                dma((depth // WIDE + 3,)), dma((3,)),
                dma((1,)), dma((n_cand,)), dma((1,)), dma((n_cand,)), dma((1,)), dma((1,)),
                dma((1,)), dma((1,)), dma((1,)), dma((1,)),
                vmem((n_pts + n_cand - 1, ta, LANES), F32), vmem((n_pts + n_cand - 1, tb, LANES), F32),
                vmem((n_pts - 1, tc, LANES), F32), vmem((n_pts - 1, 1, LANES), F32),
                pltpu.SemaphoreType.REGULAR,
            ],
            compiler_params=pltpu.CompilerParams(
                collective_id=0, has_side_effects=True, vmem_limit_bytes=60 * 2**20,
            ),
            name="facility",
        )(points, weights.reshape(tp, LANES), coverage.reshape(tp, LANES), candidates, picks)
        gains, top, cover = pl.pallas_call(
            finish,
            out_shape=(
                jax.ShapeDtypeStruct((tc, LANES), F32),
                jax.ShapeDtypeStruct((1, TOPK), F32),
                jax.ShapeDtypeStruct((tp, LANES), F32),
            ),
            in_specs=[pl.BlockSpec(memory_space=vmem)] * 3,
            out_specs=(anywhere,) * 3,
            scratch_shapes=[dma((3,))],
            name="finish",
        )(*(pltpu.with_memory_space_constraint(x, vmem) for x in (gains, top, cover)))
        return gains.reshape(cands), top.reshape(TOPK), cover.reshape(rows)

    placed = (P("pts", None), P("pts"), P("pts"), P("cand", None), P())
    return jax.shard_map(
        on_device, mesh=mesh, in_specs=placed, out_specs=(P("cand"), P(), P("pts")), check_vma=False
    )
```

```python
import functools

import jax
import jax.numpy as jnp
from jax import lax
from jax.experimental import pallas as pl
from jax.experimental.pallas import tpu as pltpu
from jax.sharding import PartitionSpec as P

TOPK = 64
LANES = 128
MESH = pl.DeviceIdType.MESH
F32 = jnp.float32
LOW = -1e30
HIGH = 3e38
WIDE = 256
PIECE = 64


def column_tile(row):
    return jnp.transpose(jnp.broadcast_to(row, (LANES, LANES)))


def kernel(
    n_pts, n_cand, points, weights, coverage, candidates, picks, gains_out, top_out, cover_out,
    p_buf, c_buf, w_buf, v_buf, k_buf, w_col, v_col, b_acc, last, part_a, part_m, part_b, parts_a, parts_m, parts_b,
    best, bests, all_gains, n_col, t_col, top_row, got_gains, got_top,
    in_sem, small_sem, a_send, a_recv, m_send, m_recv, b_send, b_recv, best_send, best_recv,
    gain_send, gain_recv, top_send, top_recv, sent_a, sent_m, sent_b, sent, heard, passed, *accs,
):
    rows, depth = points.shape
    cands = candidates.shape[0]
    me, mz = lax.axis_index("pts"), lax.axis_index("cand")
    n_k, n_c = depth // WIDE, cands // WIDE
    half = rows // 2
    pieces = half // PIECE
    tiles_p, tiles_c = rows // LANES, cands // LANES
    tiles_w = WIDE // LANES
    rows_b = tiles_w
    rows_m = tiles_w
    rows_a = tiles_c - rows_m - rows_b
    scale = depth ** (-0.5)

    steps = [(c, k) for c in range(n_c) for k in range(n_k)]
    spans = [("c", 0, 1)] + [("p", k, k + 1) for k in range(n_k)] + [("c", 1, 2), ("c", 2, n_c)]
    spans = [span for span in spans if span[1] < span[2]]
    loads = {}
    for at, (kind, first, after) in enumerate(spans):
        span = pl.ds(first * WIDE, (after - first) * WIDE)
        if kind == "p":
            src, dst = points.at[:, span], p_buf.at[:, span]
        else:
            src, dst = candidates.at[span, :], c_buf.at[span, :]
        loads[kind, first] = pltpu.make_async_copy(src, dst, in_sem.at[at])
    small = [
        pltpu.make_async_copy(weights, w_buf, small_sem.at[0]),
        pltpu.make_async_copy(coverage, v_buf, small_sem.at[1]),
        pltpu.make_async_copy(picks, k_buf, small_sem.at[2]),
    ]
    for copy in small:
        copy.start()
    for copy in loads.values():
        copy.start()

    base = mz == 0
    final = me == n_pts - 1
    ranks = base | final
    calls = final & jnp.logical_not(base)
    barrier = pltpu.get_barrier_semaphore()

    def greet(p, z):
        pl.semaphore_signal(barrier, inc=1, device_id={"pts": p, "cand": z}, device_id_type=MESH)

    @pl.when(ranks)
    def _():
        for z in range(n_cand):
            for k in range(n_pts):
                if z == 0 and k == 0:
                    continue
                greet(lax.rem(me + k, n_pts), lax.rem(mz + z, n_cand))

    for k in range(1, n_cand):
        greet(me, lax.rem(mz + k, n_cand))

    @pl.when(jnp.logical_not(ranks))
    def _():
        greet(n_pts - 1, mz)

    for copy in small:
        copy.wait()
    w_row = w_buf[...] * (scale / (rows * n_pts))
    v_row = v_buf[...] * (1.0 / scale)
    for t in range(tiles_p):
        w_col[t * LANES : (t + 1) * LANES, :] = column_tile(w_row[t : t + 1, :])
        v_col[t * LANES : (t + 1) * LANES, :] = column_tile(v_row[t : t + 1, :])
    column = mz * cands + lax.broadcasted_iota(jnp.int32, (tiles_c, LANES), 0) * LANES
    column = column + lax.broadcasted_iota(jnp.int32, (tiles_c, LANES), 1)
    chosen = jnp.zeros((tiles_c, LANES), jnp.bool_)
    for k in range(picks.shape[0]):
        chosen = chosen | (column == k_buf[k])
    penalty = jnp.where(chosen, 0.0, LOW)

    def push(at):
        c, k = steps[at]
        tile = c_buf[c * WIDE : (c + 1) * WIDE, k * WIDE : (k + 1) * WIDE]
        for q in range(2):
            pltpu.matmul_push_rhs(tile, staging_register=at % 2, mxu_index=q, transpose=True)

    def accumulator(c, i, q):
        return accs[((c % 2) * 2 + q) * pieces + i]

    def accumulate(at):
        c, k = steps[at]
        for i in range(pieces):
            for q in range(2):
                from_p = q * half + i * PIECE
                pltpu.matmul_acc_lhs(
                    accumulator(c, i, q),
                    p_buf[from_p : from_p + PIECE, k * WIDE : (k + 1) * WIDE],
                    load_staged_rhs=at % 2 if i == 0 else None,
                )

    sums = {}

    def gain_of(x, at, c, t, lane):
        value = jnp.maximum(x - v_col[at, :], 0.0) * w_col[at, :]
        key = c, t, lane
        sums[key] = sums[key] + value if key in sums else value

    def cover_of(xs, at, c):
        found = b_acc[at, :] if c else None
        for t, x in enumerate(xs):
            tile = c * tiles_w + t
            x = x + penalty[tile : tile + 1, :]
            found = x if found is None else jnp.maximum(found, x)
        b_acc[at, :] = found

    def consume(c, i, q):
        from_p = q * half + i * PIECE
        sims = pltpu.matmul_pop(accumulator(c, i, q))
        for r in range(0, PIECE, 8):
            at = slice(from_p + r, from_p + r + 8)
            xs = [sims[r : r + 8, t * LANES : (t + 1) * LANES] for t in range(tiles_w)]
            for t, x in enumerate(xs):
                gain_of(x, at, c, t, q * 2 + r // 8 % 2)
            if c + 1 < n_c:
                cover_of(xs, at, c)
            else:
                last[at, :] = sims[r : r + 8, :]

    def write_sums(c, dst, row):
        for t in range(tiles_w):
            total = (sums[c, t, 0] + sums[c, t, 1]) + (sums[c, t, 2] + sums[c, t, 3])
            dst[row + t : row + t + 1, :] = jnp.sum(total, axis=0, keepdims=True)

    def send_parts(src, slots, send, recv):
        def to(p, z):
            return pltpu.make_async_remote_copy(
                src_ref=src, dst_ref=slots.at[mz, me], send_sem=send.at[0], recv_sem=recv.at[mz],
                device_id={"pts": p, "cand": z}, device_id_type=MESH,
            )

        for k in range(n_pts - 1):
            to(k + jnp.where(base & (k >= me), 1, 0), 0).start()
        pl.when(jnp.logical_not(base))(to(n_pts - 1, 0).start)
        for z in range(1, n_cand):
            pl.when(jnp.logical_not(final & (mz == z)))(to(n_pts - 1, z).start)
        slots[mz, me] = src[...]

    loads["c", 0].wait()
    push(0)
    units = [(i, q) for i in range(pieces) for q in range(2)]
    share = len(units) // n_k
    rankers = n_pts + n_cand - 1
    awaited = (n_cand - 1) + rankers - jnp.where(ranks, 1, 0) + jnp.where(calls, n_pts - 1, 0)
    fences = []

    def fence():
        pl.semaphore_signal(passed, 1)
        fences.append(1)

    for at, (c, k) in enumerate(steps):
        if c == n_c - 1 and k == 0:
            pl.semaphore_wait(barrier, awaited)
            send_parts(part_a, parts_a, a_send, a_recv)
        elif c and k % 2 == 0:
            fence()
        if c == 0:
            loads["p", k].wait()
        if at + 1 < len(steps):
            if k + 1 == n_k and ("c", c + 1) in loads:
                loads["c", c + 1].wait()
            push(at + 1)
        accumulate(at)
        if c:
            for i, q in units[k * share : (k + 1) * share]:
                consume(c - 1, i, q)
            if k == n_k - 1:
                if c + 1 < n_c:
                    write_sums(c - 1, part_a, (c - 1) * tiles_w)
                else:
                    write_sums(c - 1, part_m, 0)

    send_parts(part_m, parts_m, m_send, m_recv)
    for at, (i, q) in enumerate(units):
        if at and at % 2 == 0:
            fence()
        consume(n_c - 1, i, q)
    write_sums(n_c - 1, part_b, 0)
    send_parts(part_b, parts_b, b_send, b_recv)
    pl.semaphore_wait(passed, len(fences))

    for r in range(0, rows, PIECE):
        at = slice(r, r + PIECE)
        cover_of([last[at, t * LANES : (t + 1) * LANES] for t in range(tiles_w)], at, n_c - 1)
    for t in range(tiles_p):
        turned = jnp.transpose(b_acc[t * LANES : (t + 1) * LANES, :])
        best[t : t + 1, :] = jnp.max(turned, axis=0, keepdims=True)
    for k in range(1, n_cand):
        pltpu.make_async_remote_copy(
            src_ref=best, dst_ref=bests.at[mz], send_sem=best_send.at[0], recv_sem=best_recv.at[0],
            device_id={"cand": lax.rem(mz + k, n_cand)}, device_id_type=MESH,
        ).start()

    def settle(view, sem):
        pltpu.make_async_copy(view, view, sem).wait()

    def finish_cover():
        settle(bests.at[pl.ds(0, n_cand - 1)], best_recv.at[0])
        cover = best[...]
        for k in range(1, n_cand):
            cover = jnp.maximum(cover, bests[lax.rem(mz + k, n_cand)])
        cover_out[...] = jnp.maximum(v_buf[...], cover * scale)
        settle(bests.at[pl.ds(0, n_cand - 1)], best_send.at[0])

    place = lax.broadcasted_iota(jnp.int32, (8, LANES), 1).astype(F32)
    lane = lax.broadcasted_iota(jnp.int32, (1, LANES), 1)

    def merge(new):
        for i, row in enumerate(new):
            n_col[i * LANES : (i + 1) * LANES, :] = column_tile(row)
        across = [jnp.broadcast_to(row, (8, LANES)) for row in new]
        across.append(jnp.broadcast_to(top_row[...], (8, LANES)))
        columns = [t_col[g * 8 : (g + 1) * 8, :] for g in range(TOPK // 8)]
        columns += [n_col[g * 8 : (g + 1) * 8, :] for g in range(len(new) * LANES // 8)]
        kept = jnp.full((8, LANES), HIGH, F32)
        for column in columns:
            above = jnp.zeros((8, LANES), F32)
            for row in across:
                above = above + jnp.where(row > column, 1.0, 0.0)
            above = jnp.sum(above, axis=1, keepdims=True)
            kept = jnp.minimum(kept, jnp.where(above <= place, column, HIGH))
        kept = jnp.min(kept, axis=0, keepdims=True)
        return jnp.where(lane < TOPK, kept, LOW)

    def told(p, src, dst, send, recv):
        return pltpu.make_async_remote_copy(
            src_ref=src, dst_ref=dst, send_sem=send.at[0], recv_sem=recv.at[0],
            device_id={"pts": p}, device_id_type=MESH,
        )

    def settle_either(fewer, view, many, sem):
        pl.when(fewer)(lambda: settle(view.at[pl.ds(0, many - 1)], sem))
        pl.when(jnp.logical_not(fewer))(lambda: settle(view.at[pl.ds(0, many)], sem))

    def settle_sends():
        settle_either(ranks, sent_a, rankers, a_send.at[0])
        settle_either(ranks, sent_m, rankers, m_send.at[0])
        settle_either(ranks, sent_b, rankers, b_send.at[0])

    def send_gains(z):
        for p in range(n_pts - 1):
            told(p, all_gains.at[z], got_gains, gain_send, gain_recv).start()

    def tell_gains(z):
        if z:
            pl.when(final & (mz == z))(lambda: send_gains(z))

    @pl.when(ranks)
    def _():
        top_row[...] = jnp.where(lane < TOPK, -1.0, LOW)
        for z in range(n_cand):
            for slots, recv, first, many in (
                (parts_a, a_recv, 0, rows_a), (parts_m, m_recv, rows_a, rows_m),
                (parts_b, b_recv, rows_a + rows_m, rows_b),
            ):
                t_col[...] = column_tile(top_row[...])[:TOPK, :]
                settle_either(mz == z, slots.at[0], n_pts, recv.at[z])
                total = slots[z, 0]
                for p in range(1, n_pts):
                    total = total + slots[z, p]
                all_gains[z, first : first + many, :] = total
                whole = first + many == tiles_c
                if whole and z + 1 < n_cand:
                    tell_gains(z)
                if whole and z == max(n_cand - 2, 0):
                    finish_cover()
                    settle_sends()
                top_row[...] = merge([total[t : t + 1, :] for t in range(many)])
        top_out[...] = top_row[:, :TOPK]
        gains_out[...] = all_gains[mz]

        @pl.when(calls)
        def _():
            for p in range(n_pts - 1):
                told(p, top_row, got_top, top_send, top_recv).start()
            pl.when(mz == n_cand - 1)(lambda: send_gains(n_cand - 1))
            settle(heard, top_send.at[0])
            settle(sent, gain_send.at[0])

    @pl.when(jnp.logical_not(ranks))
    def _():
        finish_cover()
        settle_sends()
        settle(got_gains, gain_recv.at[0])
        gains_out[...] = got_gains[...]
        settle(got_top, top_recv.at[0])
        top_out[...] = got_top[:, :TOPK]


def finish(gains, top, cover, gains_out, top_out, cover_out, sems):
    copies = [
        pltpu.make_async_copy(top, top_out, sems.at[0]),
        pltpu.make_async_copy(gains, gains_out, sems.at[1]),
        pltpu.make_async_copy(cover, cover_out, sems.at[2]),
    ]
    for copy in copies:
        copy.start()
    for copy in copies:
        copy.wait()


def solution(mesh):
    n_pts, n_cand = mesh.shape["pts"], mesh.shape["cand"]

    def on_device(points, weights, coverage, candidates, picks):
        rows, depth = points.shape
        cands = candidates.shape[0]
        tp, tc = rows // LANES, cands // LANES
        tb = WIDE // LANES
        ta = tc - 2 * tb
        anywhere = pl.BlockSpec(memory_space=pl.ANY)
        dma = pltpu.SemaphoreType.DMA
        vmem = pltpu.VMEM

        def scoped(*refs):
            many = rows // 2 // PIECE
            accs = [pltpu.ACC(q)((PIECE, WIDE), F32) for q in (0,) * many + (1,) * many] * 2
            pl.run_scoped(functools.partial(kernel, n_pts, n_cand, *refs), *accs)

        gains, top, cover = pl.pallas_call(
            scoped,
            out_shape=(vmem((tc, LANES), F32), vmem((1, TOPK), F32), vmem((tp, LANES), F32)),
            in_specs=[anywhere] * 5,
            out_specs=(pl.BlockSpec(memory_space=vmem),) * 3,
            scratch_shapes=[
                vmem((rows, depth), points.dtype), vmem((cands, depth), candidates.dtype),
                vmem((tp, LANES), F32), vmem((tp, LANES), F32),
                pltpu.SMEM(picks.shape, jnp.int32),
                vmem((rows, LANES), F32), vmem((rows, LANES), F32), vmem((rows, LANES), F32),
                vmem((rows, WIDE), F32),
                vmem((ta, LANES), F32), vmem((tb, LANES), F32), vmem((tb, LANES), F32),
                vmem((n_cand, n_pts, ta, LANES), F32), vmem((n_cand, n_pts, tb, LANES), F32),
                vmem((n_cand, n_pts, tb, LANES), F32),
                vmem((tp, LANES), F32), vmem((n_cand, tp, LANES), F32),
                vmem((n_cand, tc, LANES), F32), vmem((cands, LANES), F32), vmem((TOPK, LANES), F32),
                vmem((1, LANES), F32), vmem((tc, LANES), F32), vmem((1, LANES), F32),
                dma((depth // WIDE + 3,)), dma((3,)),
                dma((1,)), dma((n_cand,)), dma((1,)), dma((n_cand,)), dma((1,)), dma((n_cand,)),
                dma((1,)), dma((1,)),
                dma((1,)), dma((1,)), dma((1,)), dma((1,)),
                vmem((n_pts + n_cand - 1, ta, LANES), F32), vmem((n_pts + n_cand - 1, tb, LANES), F32),
                vmem((n_pts + n_cand - 1, tb, LANES), F32),
                vmem((n_pts - 1, tc, LANES), F32), vmem((n_pts - 1, 1, LANES), F32),
                pltpu.SemaphoreType.REGULAR,
            ],
            compiler_params=pltpu.CompilerParams(
                collective_id=0, has_side_effects=True, vmem_limit_bytes=60 * 2**20,
            ),
            name="facility",
        )(points, weights.reshape(tp, LANES), coverage.reshape(tp, LANES), candidates, picks)
        gains, top, cover = pl.pallas_call(
            finish,
            out_shape=(
                jax.ShapeDtypeStruct((tc, LANES), F32),
                jax.ShapeDtypeStruct((1, TOPK), F32),
                jax.ShapeDtypeStruct((tp, LANES), F32),
            ),
            in_specs=[pl.BlockSpec(memory_space=vmem)] * 3,
            out_specs=(anywhere,) * 3,
            scratch_shapes=[dma((3,))],
            name="finish",
        )(*(pltpu.with_memory_space_constraint(x, vmem) for x in (gains, top, cover)))
        return gains.reshape(cands), top.reshape(TOPK), cover.reshape(rows)

    placed = (P("pts", None), P("pts"), P("pts"), P("cand", None), P())
    return jax.shard_map(
        on_device, mesh=mesh, in_specs=placed, out_specs=(P("cand"), P(), P("pts")), check_vma=False
    )
```

```python
import functools

import jax
import jax.numpy as jnp
from jax import lax
from jax.experimental import pallas as pl
from jax.experimental.pallas import tpu as pltpu
from jax.sharding import PartitionSpec as P

TOPK = 64
LANES = 128
MESH = pl.DeviceIdType.MESH
F32 = jnp.float32
LOW = -1e30
HIGH = 3e38
WIDE = 256
PIECE = 64


def column_tile(row):
    return jnp.transpose(jnp.broadcast_to(row, (LANES, LANES)))


def kernel(
    n_pts, n_cand, points, weights, coverage, candidates, picks, gains_out, top_out, cover_out,
    p_buf, c_buf, w_buf, v_buf, k_buf, w_col, v_col, b_acc, last, part_a, part_b, parts_a, parts_b,
    best, bests, all_gains, n_col, t_col, top_row, got_gains, got_top,
    in_sem, small_sem, a_send, a_recv, b_send, b_recv, best_send, best_recv,
    gain_send, gain_recv, top_send, top_recv, sent_a, sent_b, sent, heard, passed, *accs,
):
    rows, depth = points.shape
    cands = candidates.shape[0]
    me, mz = lax.axis_index("pts"), lax.axis_index("cand")
    n_k, n_c = depth // WIDE, cands // WIDE
    half = rows // 2
    pieces = half // PIECE
    tiles_p, tiles_c = rows // LANES, cands // LANES
    tiles_w = WIDE // LANES
    rows_b = tiles_w
    rows_a = tiles_c - rows_b
    pair = 2 if n_pts % 2 == 0 else 1
    scale = depth ** (-0.5)

    steps = [(c, k) for c in range(n_c) for k in range(n_k)]
    spans = [("c", 0, 1)] + [("p", k, k + 1) for k in range(n_k)] + [("c", 1, 2), ("c", 2, n_c)]
    spans = [span for span in spans if span[1] < span[2]]
    loads = {}
    for at, (kind, first, after) in enumerate(spans):
        span = pl.ds(first * WIDE, (after - first) * WIDE)
        if kind == "p":
            src, dst = points.at[:, span], p_buf.at[:, span]
        else:
            src, dst = candidates.at[span, :], c_buf.at[span, :]
        loads[kind, first] = pltpu.make_async_copy(src, dst, in_sem.at[at])
    small = [
        pltpu.make_async_copy(weights, w_buf, small_sem.at[0]),
        pltpu.make_async_copy(coverage, v_buf, small_sem.at[1]),
        pltpu.make_async_copy(picks, k_buf, small_sem.at[2]),
    ]
    for copy in small:
        copy.start()
    for copy in loads.values():
        copy.start()

    base = mz == 0
    first_chip = me < pair
    ranks = base | first_chip
    calls = (me == pair - 1) & jnp.logical_not(base)
    barrier = pltpu.get_barrier_semaphore()

    def greet(p, z):
        pl.semaphore_signal(barrier, inc=1, device_id={"pts": p, "cand": z}, device_id_type=MESH)

    @pl.when(ranks)
    def _():
        for z in range(n_cand):
            for k in range(n_pts):
                if z == 0 and k == 0:
                    continue
                greet(lax.rem(me + k, n_pts), lax.rem(mz + z, n_cand))

    for k in range(1, n_cand):
        greet(me, lax.rem(mz + k, n_cand))

    @pl.when(jnp.logical_not(ranks))
    def _():
        greet(pair - 1, mz)

    for copy in small:
        copy.wait()
    w_row = w_buf[...] * (scale / (rows * n_pts))
    v_row = v_buf[...] * (1.0 / scale)
    for t in range(tiles_p):
        w_col[t * LANES : (t + 1) * LANES, :] = column_tile(w_row[t : t + 1, :])
        v_col[t * LANES : (t + 1) * LANES, :] = column_tile(v_row[t : t + 1, :])
    column = mz * cands + lax.broadcasted_iota(jnp.int32, (tiles_c, LANES), 0) * LANES
    column = column + lax.broadcasted_iota(jnp.int32, (tiles_c, LANES), 1)
    chosen = jnp.zeros((tiles_c, LANES), jnp.bool_)
    for k in range(picks.shape[0]):
        chosen = chosen | (column == k_buf[k])
    penalty = jnp.where(chosen, 0.0, LOW)

    def push(at):
        c, k = steps[at]
        tile = c_buf[c * WIDE : (c + 1) * WIDE, k * WIDE : (k + 1) * WIDE]
        for q in range(2):
            pltpu.matmul_push_rhs(tile, staging_register=at % 2, mxu_index=q, transpose=True)

    def accumulator(c, i, q):
        return accs[((c % 2) * 2 + q) * pieces + i]

    def accumulate(at):
        c, k = steps[at]
        for i in range(pieces):
            for q in range(2):
                from_p = q * half + i * PIECE
                pltpu.matmul_acc_lhs(
                    accumulator(c, i, q),
                    p_buf[from_p : from_p + PIECE, k * WIDE : (k + 1) * WIDE],
                    load_staged_rhs=at % 2 if i == 0 else None,
                )

    sums = {}

    def gain_of(x, at, c, t, lane):
        value = jnp.maximum(x - v_col[at, :], 0.0) * w_col[at, :]
        key = c, t, lane
        sums[key] = sums[key] + value if key in sums else value

    def cover_of(xs, at, c):
        found = b_acc[at, :] if c else None
        for t, x in enumerate(xs):
            tile = c * tiles_w + t
            x = x + penalty[tile : tile + 1, :]
            found = x if found is None else jnp.maximum(found, x)
        b_acc[at, :] = found

    def consume(c, i, q):
        from_p = q * half + i * PIECE
        sims = pltpu.matmul_pop(accumulator(c, i, q))
        for r in range(0, PIECE, 8):
            at = slice(from_p + r, from_p + r + 8)
            xs = [sims[r : r + 8, t * LANES : (t + 1) * LANES] for t in range(tiles_w)]
            for t, x in enumerate(xs):
                gain_of(x, at, c, t, q * 2 + r // 8 % 2)
            if c + 1 < n_c:
                cover_of(xs, at, c)
            else:
                last[at, :] = sims[r : r + 8, :]

    def write_sums(c, dst, row):
        for t in range(tiles_w):
            total = (sums[c, t, 0] + sums[c, t, 1]) + (sums[c, t, 2] + sums[c, t, 3])
            dst[row + t : row + t + 1, :] = jnp.sum(total, axis=0, keepdims=True)

    def send_parts(src, slots, send, recv):
        def to(p, z):
            return pltpu.make_async_remote_copy(
                src_ref=src, dst_ref=slots.at[mz, me], send_sem=send.at[0], recv_sem=recv.at[mz],
                device_id={"pts": p, "cand": z}, device_id_type=MESH,
            )

        for k in range(n_pts - 1):
            to(k + jnp.where(base & (k >= me), 1, 0), 0).start()
        pl.when(jnp.logical_not(base))(to(n_pts - 1, 0).start)
        for z in range(1, n_cand):
            for p in range(pair):
                pl.when(jnp.logical_not((me == p) & (mz == z)))(to(p, z).start)
        slots[mz, me] = src[...]

    loads["c", 0].wait()
    push(0)
    units = [(i, q) for i in range(pieces) for q in range(2)]
    share = len(units) // n_k
    fences = []

    def fence():
        pl.semaphore_signal(passed, 1)
        fences.append(1)

    for at, (c, k) in enumerate(steps):
        if c and k % 2 == 0:
            fence()
        if c == 0:
            loads["p", k].wait()
        if at + 1 < len(steps):
            if k + 1 == n_k and ("c", c + 1) in loads:
                loads["c", c + 1].wait()
            push(at + 1)
        accumulate(at)
        if c:
            for i, q in units[k * share : (k + 1) * share]:
                consume(c - 1, i, q)
            if k == n_k - 1:
                write_sums(c - 1, part_a, (c - 1) * tiles_w)

    rankers = n_pts + pair * (n_cand - 1)
    awaited = (n_cand - 1) + rankers - jnp.where(ranks, 1, 0) + jnp.where(calls, n_pts - pair, 0)
    pl.semaphore_wait(barrier, awaited)
    send_parts(part_a, parts_a, a_send, a_recv)
    for at, (i, q) in enumerate(units):
        if at and at % 2 == 0:
            fence()
        consume(n_c - 1, i, q)
    write_sums(n_c - 1, part_b, 0)
    send_parts(part_b, parts_b, b_send, b_recv)
    pl.semaphore_wait(passed, len(fences))

    for r in range(0, rows, PIECE):
        at = slice(r, r + PIECE)
        cover_of([last[at, t * LANES : (t + 1) * LANES] for t in range(tiles_w)], at, n_c - 1)
    for t in range(tiles_p):
        turned = jnp.transpose(b_acc[t * LANES : (t + 1) * LANES, :])
        best[t : t + 1, :] = jnp.max(turned, axis=0, keepdims=True)
    for k in range(1, n_cand):
        pltpu.make_async_remote_copy(
            src_ref=best, dst_ref=bests.at[mz], send_sem=best_send.at[0], recv_sem=best_recv.at[0],
            device_id={"cand": lax.rem(mz + k, n_cand)}, device_id_type=MESH,
        ).start()

    def settle(view, sem):
        pltpu.make_async_copy(view, view, sem).wait()

    def finish_cover():
        settle(bests.at[pl.ds(0, n_cand - 1)], best_recv.at[0])
        cover = best[...]
        for k in range(1, n_cand):
            cover = jnp.maximum(cover, bests[lax.rem(mz + k, n_cand)])
        cover_out[...] = jnp.maximum(v_buf[...], cover * scale)
        settle(bests.at[pl.ds(0, n_cand - 1)], best_send.at[0])

    place = lax.broadcasted_iota(jnp.int32, (8, LANES), 1).astype(F32)
    lane = lax.broadcasted_iota(jnp.int32, (1, LANES), 1)

    def merge(new):
        for i, row in enumerate(new):
            n_col[i * LANES : (i + 1) * LANES, :] = column_tile(row)
        across = [jnp.broadcast_to(row, (8, LANES)) for row in new]
        across.append(jnp.broadcast_to(top_row[...], (8, LANES)))
        columns = [t_col[g * 8 : (g + 1) * 8, :] for g in range(TOPK // 8)]
        columns += [n_col[g * 8 : (g + 1) * 8, :] for g in range(len(new) * LANES // 8)]
        kept = jnp.full((8, LANES), HIGH, F32)
        for column in columns:
            above = jnp.zeros((8, LANES), F32)
            for row in across:
                above = above + jnp.where(row > column, 1.0, 0.0)
            above = jnp.sum(above, axis=1, keepdims=True)
            kept = jnp.minimum(kept, jnp.where(above <= place, column, HIGH))
        kept = jnp.min(kept, axis=0, keepdims=True)
        return jnp.where(lane < TOPK, kept, LOW)

    def told(p, src, dst, send, recv):
        return pltpu.make_async_remote_copy(
            src_ref=src, dst_ref=dst, send_sem=send.at[0], recv_sem=recv.at[0],
            device_id={"pts": p}, device_id_type=MESH,
        )

    def settle_either(fewer, view, many, sem):
        pl.when(fewer)(lambda: settle(view.at[pl.ds(0, many - 1)], sem))
        pl.when(jnp.logical_not(fewer))(lambda: settle(view.at[pl.ds(0, many)], sem))

    def settle_sends():
        settle_either(ranks, sent_a, rankers, a_send.at[0])
        settle_either(ranks, sent_b, rankers, b_send.at[0])

    def send_gains(z):
        for p in range(pair, n_pts):
            told(p, all_gains.at[z], got_gains, gain_send, gain_recv).start()

    def tell_gains(z):
        if z:
            pl.when(calls & (mz == z))(lambda: send_gains(z))

    @pl.when(ranks)
    def _():
        top_row[...] = jnp.where(lane < TOPK, -1.0, LOW)
        for z in range(n_cand):
            for slots, recv, first, many in (
                (parts_a, a_recv, 0, rows_a), (parts_b, b_recv, rows_a, rows_b)
            ):
                if not first:
                    t_col[...] = column_tile(top_row[...])[:TOPK, :]
                settle_either(mz == z, slots.at[0], n_pts, recv.at[z])
                if first:
                    t_col[...] = column_tile(top_row[...])[:TOPK, :]
                total = slots[z, 0]
                for p in range(1, n_pts):
                    total = total + slots[z, p]
                all_gains[z, first : first + many, :] = total
                if first and z + 1 < n_cand:
                    tell_gains(z)
                if first and z == max(n_cand - 2, 0):
                    finish_cover()
                    settle_sends()
                top_row[...] = merge([total[t : t + 1, :] for t in range(many)])
        top_out[...] = top_row[:, :TOPK]
        gains_out[...] = all_gains[mz]

        @pl.when(calls)
        def _():
            for p in range(pair, n_pts):
                told(p, top_row, got_top, top_send, top_recv).start()
            pl.when(mz == n_cand - 1)(lambda: send_gains(n_cand - 1))
            settle(heard, top_send.at[0])
            settle(sent, gain_send.at[0])

    @pl.when(jnp.logical_not(ranks))
    def _():
        finish_cover()
        settle_sends()
        settle(got_gains, gain_recv.at[0])
        gains_out[...] = got_gains[...]
        settle(got_top, top_recv.at[0])
        top_out[...] = got_top[:, :TOPK]


def finish(gains, top, cover, gains_out, top_out, cover_out, sems):
    copies = [
        pltpu.make_async_copy(top, top_out, sems.at[0]),
        pltpu.make_async_copy(gains, gains_out, sems.at[1]),
        pltpu.make_async_copy(cover, cover_out, sems.at[2]),
    ]
    for copy in copies:
        copy.start()
    for copy in copies:
        copy.wait()


def solution(mesh):
    n_pts, n_cand = mesh.shape["pts"], mesh.shape["cand"]

    def on_device(points, weights, coverage, candidates, picks):
        rows, depth = points.shape
        cands = candidates.shape[0]
        tp, tc = rows // LANES, cands // LANES
        tb = WIDE // LANES
        ta = tc - tb
        pair = 2 if n_pts % 2 == 0 else 1
        anywhere = pl.BlockSpec(memory_space=pl.ANY)
        dma = pltpu.SemaphoreType.DMA
        vmem = pltpu.VMEM

        def scoped(*refs):
            many = rows // 2 // PIECE
            accs = [pltpu.ACC(q)((PIECE, WIDE), F32) for q in (0,) * many + (1,) * many] * 2
            pl.run_scoped(functools.partial(kernel, n_pts, n_cand, *refs), *accs)

        gains, top, cover = pl.pallas_call(
            scoped,
            out_shape=(vmem((tc, LANES), F32), vmem((1, TOPK), F32), vmem((tp, LANES), F32)),
            in_specs=[anywhere] * 5,
            out_specs=(pl.BlockSpec(memory_space=vmem),) * 3,
            scratch_shapes=[
                vmem((rows, depth), points.dtype), vmem((cands, depth), candidates.dtype),
                vmem((tp, LANES), F32), vmem((tp, LANES), F32),
                pltpu.SMEM(picks.shape, jnp.int32),
                vmem((rows, LANES), F32), vmem((rows, LANES), F32), vmem((rows, LANES), F32),
                vmem((rows, WIDE), F32),
                vmem((ta, LANES), F32), vmem((tb, LANES), F32),
                vmem((n_cand, n_pts, ta, LANES), F32), vmem((n_cand, n_pts, tb, LANES), F32),
                vmem((tp, LANES), F32), vmem((n_cand, tp, LANES), F32),
                vmem((n_cand, tc, LANES), F32), vmem((cands, LANES), F32), vmem((TOPK, LANES), F32),
                vmem((1, LANES), F32), vmem((tc, LANES), F32), vmem((1, LANES), F32),
                dma((depth // WIDE + 3,)), dma((3,)),
                dma((1,)), dma((n_cand,)), dma((1,)), dma((n_cand,)), dma((1,)), dma((1,)),
                dma((1,)), dma((1,)), dma((1,)), dma((1,)),
                vmem((n_pts + pair * (n_cand - 1), ta, LANES), F32), vmem((n_pts + pair * (n_cand - 1), tb, LANES), F32),
                vmem((n_pts - pair, tc, LANES), F32), vmem((n_pts - pair, 1, LANES), F32),
                pltpu.SemaphoreType.REGULAR,
            ],
            compiler_params=pltpu.CompilerParams(
                collective_id=0, has_side_effects=True, vmem_limit_bytes=60 * 2**20,
            ),
            name="facility",
        )(points, weights.reshape(tp, LANES), coverage.reshape(tp, LANES), candidates, picks)
        gains, top, cover = pl.pallas_call(
            finish,
            out_shape=(
                jax.ShapeDtypeStruct((tc, LANES), F32),
                jax.ShapeDtypeStruct((1, TOPK), F32),
                jax.ShapeDtypeStruct((tp, LANES), F32),
            ),
            in_specs=[pl.BlockSpec(memory_space=vmem)] * 3,
            out_specs=(anywhere,) * 3,
            scratch_shapes=[dma((3,))],
            name="finish",
        )(*(pltpu.with_memory_space_constraint(x, vmem) for x in (gains, top, cover)))
        return gains.reshape(cands), top.reshape(TOPK), cover.reshape(rows)

    placed = (P("pts", None), P("pts"), P("pts"), P("cand", None), P())
    return jax.shard_map(
        on_device, mesh=mesh, in_specs=placed, out_specs=(P("cand"), P(), P("pts")), check_vma=False
    )
```

```python
import functools

import jax
import jax.numpy as jnp
from jax import lax
from jax.experimental import pallas as pl
from jax.experimental.pallas import tpu as pltpu
from jax.sharding import PartitionSpec as P

TOPK = 64
LANES = 128
MESH = pl.DeviceIdType.MESH
F32 = jnp.float32
LOW = -1e30
HIGH = 3e38
WIDE = 256
PIECE = 64


def column_tile(row):
    return jnp.transpose(jnp.broadcast_to(row, (LANES, LANES)))


def kernel(
    n_pts, n_cand, points, weights, coverage, candidates, picks, gains_out, top_out, cover_out,
    p_buf, c_buf, w_buf, v_buf, k_buf, w_col, v_col, b_acc, last, part_a, part_b, parts_a, parts_b,
    best, bests, all_gains, n_col, t_col, top_row, got_gains, got_top,
    in_sem, small_sem, a_send, a_recv, b_send, b_recv, best_send, best_recv,
    gain_send, gain_recv, top_send, top_recv, sent_a, sent_b, sent, heard, passed, *accs,
):
    rows, depth = points.shape
    cands = candidates.shape[0]
    me, mz = lax.axis_index("pts"), lax.axis_index("cand")
    n_k, n_c = depth // WIDE, cands // WIDE
    half = rows // 2
    pieces = half // PIECE
    tiles_p, tiles_c = rows // LANES, cands // LANES
    tiles_w = WIDE // LANES
    rows_b = tiles_w
    rows_a = tiles_c - rows_b
    pair = 2 if n_pts % 2 == 0 else 1
    scale = depth ** (-0.5)

    steps = [(c, k) for c in range(n_c) for k in range(n_k)]
    spans = [("c", 0, 1)] + [("p", k, k + 1) for k in range(n_k)] + [("c", 1, 2), ("c", 2, n_c)]
    spans = [span for span in spans if span[1] < span[2]]
    loads = {}
    for at, (kind, first, after) in enumerate(spans):
        span = pl.ds(first * WIDE, (after - first) * WIDE)
        if kind == "p":
            src, dst = points.at[:, span], p_buf.at[:, span]
        else:
            src, dst = candidates.at[span, :], c_buf.at[span, :]
        loads[kind, first] = pltpu.make_async_copy(src, dst, in_sem.at[at])
    small = [
        pltpu.make_async_copy(weights, w_buf, small_sem.at[0]),
        pltpu.make_async_copy(coverage, v_buf, small_sem.at[1]),
        pltpu.make_async_copy(picks, k_buf, small_sem.at[2]),
    ]
    for copy in small:
        copy.start()
    for copy in loads.values():
        copy.start()

    base = mz == 0
    told_by = me == pair - 1
    ranks = base | told_by
    calls = told_by & jnp.logical_not(base)
    barrier = pltpu.get_barrier_semaphore()

    def greet(p, z):
        pl.semaphore_signal(barrier, inc=1, device_id={"pts": p, "cand": z}, device_id_type=MESH)

    @pl.when(ranks)
    def _():
        for z in range(n_cand):
            for k in range(n_pts):
                if z == 0 and k == 0:
                    continue
                greet(lax.rem(me + k, n_pts), lax.rem(mz + z, n_cand))

    for k in range(1, n_cand):
        greet(me, lax.rem(mz + k, n_cand))

    @pl.when(jnp.logical_not(ranks))
    def _():
        greet(pair - 1, mz)

    for copy in small:
        copy.wait()
    w_row = w_buf[...] * (scale / (rows * n_pts))
    v_row = v_buf[...] * (1.0 / scale)
    for t in range(tiles_p):
        w_col[t * LANES : (t + 1) * LANES, :] = column_tile(w_row[t : t + 1, :])
        v_col[t * LANES : (t + 1) * LANES, :] = column_tile(v_row[t : t + 1, :])
    column = mz * cands + lax.broadcasted_iota(jnp.int32, (tiles_c, LANES), 0) * LANES
    column = column + lax.broadcasted_iota(jnp.int32, (tiles_c, LANES), 1)
    chosen = jnp.zeros((tiles_c, LANES), jnp.bool_)
    for k in range(picks.shape[0]):
        chosen = chosen | (column == k_buf[k])
    penalty = jnp.where(chosen, 0.0, LOW)

    def push(at):
        c, k = steps[at]
        tile = c_buf[c * WIDE : (c + 1) * WIDE, k * WIDE : (k + 1) * WIDE]
        for q in range(2):
            pltpu.matmul_push_rhs(tile, staging_register=at % 2, mxu_index=q, transpose=True)

    def accumulator(c, i, q):
        return accs[((c % 2) * 2 + q) * pieces + i]

    def accumulate(at):
        c, k = steps[at]
        for i in range(pieces):
            for q in range(2):
                from_p = q * half + i * PIECE
                pltpu.matmul_acc_lhs(
                    accumulator(c, i, q),
                    p_buf[from_p : from_p + PIECE, k * WIDE : (k + 1) * WIDE],
                    load_staged_rhs=at % 2 if i == 0 else None,
                )

    sums = {}

    def gain_of(x, at, c, t, lane):
        value = jnp.maximum(x - v_col[at, :], 0.0) * w_col[at, :]
        key = c, t, lane
        sums[key] = sums[key] + value if key in sums else value

    def cover_of(xs, at, c):
        found = b_acc[at, :] if c else None
        for t, x in enumerate(xs):
            tile = c * tiles_w + t
            x = x + penalty[tile : tile + 1, :]
            found = x if found is None else jnp.maximum(found, x)
        b_acc[at, :] = found

    def consume(c, i, q):
        from_p = q * half + i * PIECE
        sims = pltpu.matmul_pop(accumulator(c, i, q))
        for r in range(0, PIECE, 8):
            at = slice(from_p + r, from_p + r + 8)
            xs = [sims[r : r + 8, t * LANES : (t + 1) * LANES] for t in range(tiles_w)]
            for t, x in enumerate(xs):
                gain_of(x, at, c, t, q * 2 + r // 8 % 2)
            if c + 1 < n_c:
                cover_of(xs, at, c)
            else:
                last[at, :] = sims[r : r + 8, :]

    def write_sums(c, dst, row):
        for t in range(tiles_w):
            total = (sums[c, t, 0] + sums[c, t, 1]) + (sums[c, t, 2] + sums[c, t, 3])
            dst[row + t : row + t + 1, :] = jnp.sum(total, axis=0, keepdims=True)

    def sends(src, slots, send, recv):
        def to(p, z):
            return pltpu.make_async_remote_copy(
                src_ref=src, dst_ref=slots.at[mz, me], send_sem=send.at[0], recv_sem=recv.at[mz],
                device_id={"pts": p, "cand": z}, device_id_type=MESH,
            )

        def unless(skipped, copy):
            return lambda: pl.when(jnp.logical_not(skipped))(copy.start)

        def keep():
            slots[mz, me] = src[...]

        work = [to(k + jnp.where(base & (k >= me), 1, 0), 0).start for k in range(n_pts - 1)]
        work.append(unless(base, to(n_pts - 1, 0)))
        for z in range(1, n_cand):
            work.append(unless(told_by & (mz == z), to(pair - 1, z)))
        return work + [keep]

    loads["c", 0].wait()
    push(0)
    units = [(i, q) for i in range(pieces) for q in range(2)]
    share = len(units) // n_k
    fences = []

    def fence():
        pl.semaphore_signal(passed, 1)
        fences.append(1)

    for at, (c, k) in enumerate(steps):
        if c and k % 2 == 0:
            fence()
        if c == 0:
            loads["p", k].wait()
        if at + 1 < len(steps):
            if k + 1 == n_k and ("c", c + 1) in loads:
                loads["c", c + 1].wait()
            push(at + 1)
        accumulate(at)
        if c:
            for i, q in units[k * share : (k + 1) * share]:
                consume(c - 1, i, q)
            if k == n_k - 1:
                write_sums(c - 1, part_a, (c - 1) * tiles_w)

    rankers = n_pts + n_cand - 1
    awaited = (n_cand - 1) + rankers - jnp.where(ranks, 1, 0) + jnp.where(calls, n_pts - 1, 0)
    pl.semaphore_wait(barrier, awaited)
    early = sends(part_a, parts_a, a_send, a_recv)
    early.pop(0)()
    early.pop(0)()
    for at, (i, q) in enumerate(units):
        if at and at % 2 == 0:
            fence()
        consume(n_c - 1, i, q)
        for _ in range(-(-len(early) // (len(units) - at))):
            early.pop(0)()
    write_sums(n_c - 1, part_b, 0)
    for one in sends(part_b, parts_b, b_send, b_recv):
        one()
    pl.semaphore_wait(passed, len(fences))

    for r in range(0, rows, PIECE):
        at = slice(r, r + PIECE)
        cover_of([last[at, t * LANES : (t + 1) * LANES] for t in range(tiles_w)], at, n_c - 1)
    for t in range(tiles_p):
        turned = jnp.transpose(b_acc[t * LANES : (t + 1) * LANES, :])
        best[t : t + 1, :] = jnp.max(turned, axis=0, keepdims=True)
    for k in range(1, n_cand):
        pltpu.make_async_remote_copy(
            src_ref=best, dst_ref=bests.at[mz], send_sem=best_send.at[0], recv_sem=best_recv.at[0],
            device_id={"cand": lax.rem(mz + k, n_cand)}, device_id_type=MESH,
        ).start()

    def settle(view, sem):
        pltpu.make_async_copy(view, view, sem).wait()

    def finish_cover():
        settle(bests.at[pl.ds(0, n_cand - 1)], best_recv.at[0])
        cover = best[...]
        for k in range(1, n_cand):
            cover = jnp.maximum(cover, bests[lax.rem(mz + k, n_cand)])
        cover_out[...] = jnp.maximum(v_buf[...], cover * scale)
        settle(bests.at[pl.ds(0, n_cand - 1)], best_send.at[0])

    place = lax.broadcasted_iota(jnp.int32, (8, LANES), 1).astype(F32)
    lane = lax.broadcasted_iota(jnp.int32, (1, LANES), 1)

    def merge(new):
        for i, row in enumerate(new):
            n_col[i * LANES : (i + 1) * LANES, :] = column_tile(row)
        across = [jnp.broadcast_to(row, (8, LANES)) for row in new]
        across.append(jnp.broadcast_to(top_row[...], (8, LANES)))
        columns = [t_col[g * 8 : (g + 1) * 8, :] for g in range(TOPK // 8)]
        columns += [n_col[g * 8 : (g + 1) * 8, :] for g in range(len(new) * LANES // 8)]
        kept = jnp.full((8, LANES), HIGH, F32)
        for column in columns:
            above = jnp.zeros((8, LANES), F32)
            for row in across:
                above = above + jnp.where(row > column, 1.0, 0.0)
            above = jnp.sum(above, axis=1, keepdims=True)
            kept = jnp.minimum(kept, jnp.where(above <= place, column, HIGH))
        kept = jnp.min(kept, axis=0, keepdims=True)
        return jnp.where(lane < TOPK, kept, LOW)

    def told(p, src, dst, send, recv):
        return pltpu.make_async_remote_copy(
            src_ref=src, dst_ref=dst, send_sem=send.at[0], recv_sem=recv.at[0],
            device_id={"pts": p}, device_id_type=MESH,
        )

    def settle_either(fewer, view, many, sem):
        pl.when(fewer)(lambda: settle(view.at[pl.ds(0, many - 1)], sem))
        pl.when(jnp.logical_not(fewer))(lambda: settle(view.at[pl.ds(0, many)], sem))

    def settle_sends():
        settle_either(ranks, sent_a, rankers, a_send.at[0])
        settle_either(ranks, sent_b, rankers, b_send.at[0])

    def tell_all(src, dst, send, recv, here):
        def tell(k, carry):
            told(lax.rem(me + k, n_pts), src, dst, send, recv).start()
            return carry

        lax.fori_loop(1, jnp.where(here, n_pts, 1), tell, 0)

    def tell_gains(z):
        if z:
            tell_all(all_gains.at[z], got_gains, gain_send, gain_recv, calls & (mz == z))

    @pl.when(ranks)
    def _():
        top_row[...] = jnp.where(lane < TOPK, -1.0, LOW)
        for z in range(n_cand):
            for slots, recv, first, many in (
                (parts_a, a_recv, 0, rows_a), (parts_b, b_recv, rows_a, rows_b)
            ):
                if not first:
                    t_col[...] = column_tile(top_row[...])[:TOPK, :]
                settle_either(mz == z, slots.at[0], n_pts, recv.at[z])
                if first:
                    t_col[...] = column_tile(top_row[...])[:TOPK, :]
                total = slots[z, 0]
                for p in range(1, n_pts):
                    total = total + slots[z, p]
                all_gains[z, first : first + many, :] = total
                if first and z + 1 < n_cand:
                    tell_gains(z)
                if first and z + 1 == n_cand:
                    gains_out[...] = all_gains[mz]
                if first and z == max(n_cand - 2, 0):
                    finish_cover()
                    settle_sends()
                top_row[...] = merge([total[t : t + 1, :] for t in range(many)])
        top_out[...] = top_row[:, :TOPK]
        tell_all(top_row, got_top, top_send, top_recv, calls)
        tell_gains(n_cand - 1)

        def drain(k, carry):
            settle(heard, top_send.at[0])
            settle(sent, gain_send.at[0])
            return carry

        lax.fori_loop(0, jnp.where(calls, 1, 0), drain, 0)

    @pl.when(jnp.logical_not(ranks))
    def _():
        finish_cover()
        settle_sends()
        settle(got_gains, gain_recv.at[0])
        gains_out[...] = got_gains[...]
        settle(got_top, top_recv.at[0])
        top_out[...] = got_top[:, :TOPK]


def finish(gains, top, cover, gains_out, top_out, cover_out, sems):
    copies = [
        pltpu.make_async_copy(top, top_out, sems.at[0]),
        pltpu.make_async_copy(gains, gains_out, sems.at[1]),
        pltpu.make_async_copy(cover, cover_out, sems.at[2]),
    ]
    for copy in copies:
        copy.start()
    for copy in copies:
        copy.wait()


def solution(mesh):
    n_pts, n_cand = mesh.shape["pts"], mesh.shape["cand"]

    def on_device(points, weights, coverage, candidates, picks):
        rows, depth = points.shape
        cands = candidates.shape[0]
        tp, tc = rows // LANES, cands // LANES
        tb = WIDE // LANES
        ta = tc - tb
        anywhere = pl.BlockSpec(memory_space=pl.ANY)
        dma = pltpu.SemaphoreType.DMA
        vmem = pltpu.VMEM

        def scoped(*refs):
            many = rows // 2 // PIECE
            accs = [pltpu.ACC(q)((PIECE, WIDE), F32) for q in (0,) * many + (1,) * many] * 2
            pl.run_scoped(functools.partial(kernel, n_pts, n_cand, *refs), *accs)

        gains, top, cover = pl.pallas_call(
            scoped,
            out_shape=(vmem((tc, LANES), F32), vmem((1, TOPK), F32), vmem((tp, LANES), F32)),
            in_specs=[anywhere] * 5,
            out_specs=(pl.BlockSpec(memory_space=vmem),) * 3,
            scratch_shapes=[
                vmem((rows, depth), points.dtype), vmem((cands, depth), candidates.dtype),
                vmem((tp, LANES), F32), vmem((tp, LANES), F32),
                pltpu.SMEM(picks.shape, jnp.int32),
                vmem((rows, LANES), F32), vmem((rows, LANES), F32), vmem((rows, LANES), F32),
                vmem((rows, WIDE), F32),
                vmem((ta, LANES), F32), vmem((tb, LANES), F32),
                vmem((n_cand, n_pts, ta, LANES), F32), vmem((n_cand, n_pts, tb, LANES), F32),
                vmem((tp, LANES), F32), vmem((n_cand, tp, LANES), F32),
                vmem((n_cand, tc, LANES), F32), vmem((cands, LANES), F32), vmem((TOPK, LANES), F32),
                vmem((1, LANES), F32), vmem((tc, LANES), F32), vmem((1, LANES), F32),
                dma((depth // WIDE + 3,)), dma((3,)),
                dma((1,)), dma((n_cand,)), dma((1,)), dma((n_cand,)), dma((1,)), dma((1,)),
                dma((1,)), dma((1,)), dma((1,)), dma((1,)),
                vmem((n_pts + n_cand - 1, ta, LANES), F32), vmem((n_pts + n_cand - 1, tb, LANES), F32),
                vmem((n_pts - 1, tc, LANES), F32), vmem((n_pts - 1, 1, LANES), F32),
                pltpu.SemaphoreType.REGULAR,
            ],
            compiler_params=pltpu.CompilerParams(
                collective_id=0, has_side_effects=True, vmem_limit_bytes=60 * 2**20,
            ),
            name="facility",
        )(points, weights.reshape(tp, LANES), coverage.reshape(tp, LANES), candidates, picks)
        gains, top, cover = pl.pallas_call(
            finish,
            out_shape=(
                jax.ShapeDtypeStruct((tc, LANES), F32),
                jax.ShapeDtypeStruct((1, TOPK), F32),
                jax.ShapeDtypeStruct((tp, LANES), F32),
            ),
            in_specs=[pl.BlockSpec(memory_space=vmem)] * 3,
            out_specs=(anywhere,) * 3,
            scratch_shapes=[dma((3,))],
            name="finish",
        )(*(pltpu.with_memory_space_constraint(x, vmem) for x in (gains, top, cover)))
        return gains.reshape(cands), top.reshape(TOPK), cover.reshape(rows)

    placed = (P("pts", None), P("pts"), P("pts"), P("cand", None), P())
    return jax.shard_map(
        on_device, mesh=mesh, in_specs=placed, out_specs=(P("cand"), P(), P("pts")), check_vma=False
    )
```

```python
import functools

import jax
import jax.numpy as jnp
from jax import lax
from jax.experimental import pallas as pl
from jax.experimental.pallas import tpu as pltpu
from jax.sharding import PartitionSpec as P

TOPK = 64
LANES = 128
MESH = pl.DeviceIdType.MESH
F32 = jnp.float32
LOW = -1e30
HIGH = 3e38
WIDE = 256
PIECE = 64


def column_tile(row):
    return jnp.transpose(jnp.broadcast_to(row, (LANES, LANES)))


def kernel(
    n_pts, n_cand, points, weights, coverage, candidates, picks, gains_out, top_out, cover_out,
    p_buf, c_buf, w_buf, v_buf, k_buf, w_col, v_col, b_acc, last, part_a, part_b, parts_a, parts_b,
    best, bests, all_gains, n_col, t_col, top_row, got_gains, got_top,
    in_sem, small_sem, a_recv, b_recv, best_recv, gain_recv, top_recv, sent_a, sent_b, sent, heard, passed, *accs,
):
    rows, depth = points.shape
    cands = candidates.shape[0]
    me, mz = lax.axis_index("pts"), lax.axis_index("cand")
    n_k, n_c = depth // WIDE, cands // WIDE
    half = rows // 2
    pieces = half // PIECE
    tiles_p, tiles_c = rows // LANES, cands // LANES
    tiles_w = WIDE // LANES
    rows_b = tiles_w
    rows_a = tiles_c - rows_b
    a_send, b_send, best_send, gain_send, top_send = (in_sem.at[pl.ds(i, 1)] for i in range(5))
    pair = 2 if n_pts % 2 == 0 else 1
    scale = depth ** (-0.5)

    steps = [(c, k) for c in range(n_c) for k in range(n_k)]
    spans = [("c", 0, 1)] + [("p", k, k + 1) for k in range(n_k)] + [("c", 1, 2), ("c", 2, n_c)]
    spans = [span for span in spans if span[1] < span[2]]
    loads = {}
    for at, (kind, first, after) in enumerate(spans):
        span = pl.ds(first * WIDE, (after - first) * WIDE)
        if kind == "p":
            src, dst = points.at[:, span], p_buf.at[:, span]
        else:
            src, dst = candidates.at[span, :], c_buf.at[span, :]
        loads[kind, first] = pltpu.make_async_copy(src, dst, in_sem.at[at])
    small = [
        pltpu.make_async_copy(weights, w_buf, small_sem.at[0]),
        pltpu.make_async_copy(coverage, v_buf, small_sem.at[1]),
        pltpu.make_async_copy(picks, k_buf, small_sem.at[2]),
    ]
    for copy in small:
        copy.start()
    for copy in loads.values():
        copy.start()

    base = mz == 0
    told_by = me == pair - 1
    ranks = base | told_by
    calls = told_by & jnp.logical_not(base)
    barrier = pltpu.get_barrier_semaphore()

    def greet(p, z):
        pl.semaphore_signal(barrier, inc=1, device_id={"pts": p, "cand": z}, device_id_type=MESH)

    @pl.when(ranks)
    def _():
        for z in range(n_cand):
            for k in range(n_pts):
                if z == 0 and k == 0:
                    continue
                greet(lax.rem(me + k, n_pts), lax.rem(mz + z, n_cand))

    for k in range(1, n_cand):
        greet(me, lax.rem(mz + k, n_cand))

    @pl.when(jnp.logical_not(ranks))
    def _():
        greet(pair - 1, mz)

    for copy in small:
        copy.wait()
    w_row = w_buf[...] * (scale / (rows * n_pts))
    v_row = v_buf[...] * (1.0 / scale)
    for t in range(tiles_p):
        w_col[t * LANES : (t + 1) * LANES, :] = column_tile(w_row[t : t + 1, :])
        v_col[t * LANES : (t + 1) * LANES, :] = column_tile(v_row[t : t + 1, :])
    column = mz * cands + lax.broadcasted_iota(jnp.int32, (tiles_c, LANES), 0) * LANES
    column = column + lax.broadcasted_iota(jnp.int32, (tiles_c, LANES), 1)
    chosen = jnp.zeros((tiles_c, LANES), jnp.bool_)
    for k in range(picks.shape[0]):
        chosen = chosen | (column == k_buf[k])
    penalty = jnp.where(chosen, 0.0, LOW)

    def push(at):
        c, k = steps[at]
        tile = c_buf[c * WIDE : (c + 1) * WIDE, k * WIDE : (k + 1) * WIDE]
        for q in range(2):
            pltpu.matmul_push_rhs(tile, staging_register=at % 2, mxu_index=q, transpose=True)

    def accumulator(c, i, q):
        return accs[((c % 2) * 2 + q) * pieces + i]

    def accumulate(at):
        c, k = steps[at]
        for i in range(pieces):
            for q in range(2):
                from_p = q * half + i * PIECE
                pltpu.matmul_acc_lhs(
                    accumulator(c, i, q),
                    p_buf[from_p : from_p + PIECE, k * WIDE : (k + 1) * WIDE],
                    load_staged_rhs=at % 2 if i == 0 else None,
                )

    sums = {}

    def gain_of(x, at, c, t, lane):
        value = jnp.maximum(x - v_col[at, :], 0.0) * w_col[at, :]
        key = c, t, lane
        sums[key] = sums[key] + value if key in sums else value

    def cover_of(xs, at, c):
        found = b_acc[at, :] if c else None
        for t, x in enumerate(xs):
            tile = c * tiles_w + t
            x = x + penalty[tile : tile + 1, :]
            found = x if found is None else jnp.maximum(found, x)
        b_acc[at, :] = found

    def consume(c, i, q):
        from_p = q * half + i * PIECE
        sims = pltpu.matmul_pop(accumulator(c, i, q))
        for r in range(0, PIECE, 8):
            at = slice(from_p + r, from_p + r + 8)
            xs = [sims[r : r + 8, t * LANES : (t + 1) * LANES] for t in range(tiles_w)]
            for t, x in enumerate(xs):
                gain_of(x, at, c, t, q * 2 + r // 8 % 2)
            if c + 1 < n_c:
                cover_of(xs, at, c)
            else:
                last[at, :] = sims[r : r + 8, :]

    def write_sums(c, dst, row):
        for t in range(tiles_w):
            total = (sums[c, t, 0] + sums[c, t, 1]) + (sums[c, t, 2] + sums[c, t, 3])
            dst[row + t : row + t + 1, :] = jnp.sum(total, axis=0, keepdims=True)

    def sends(src, slots, send, recv):
        def to(p, z):
            return pltpu.make_async_remote_copy(
                src_ref=src, dst_ref=slots.at[mz, me], send_sem=send.at[0], recv_sem=recv.at[mz],
                device_id={"pts": p, "cand": z}, device_id_type=MESH,
            )

        def unless(skipped, copy):
            return lambda: pl.when(jnp.logical_not(skipped))(copy.start)

        def keep():
            slots[mz, me] = src[...]

        work = [to(k + jnp.where(base & (k >= me), 1, 0), 0).start for k in range(n_pts - 1)]
        work.append(unless(base, to(n_pts - 1, 0)))
        for z in range(1, n_cand):
            work.append(unless(told_by & (mz == z), to(pair - 1, z)))
        return work + [keep]

    loads["c", 0].wait()
    push(0)
    units = [(i, q) for i in range(pieces) for q in range(2)]
    share = len(units) // n_k
    fences = []

    def fence():
        pl.semaphore_signal(passed, 1)
        fences.append(1)

    for at, (c, k) in enumerate(steps):
        if c and k % 2 == 0:
            fence()
        if c == 0:
            loads["p", k].wait()
        if at + 1 < len(steps):
            if k + 1 == n_k and ("c", c + 1) in loads:
                loads["c", c + 1].wait()
            push(at + 1)
        accumulate(at)
        if c:
            for i, q in units[k * share : (k + 1) * share]:
                consume(c - 1, i, q)
            if k == n_k - 1:
                write_sums(c - 1, part_a, (c - 1) * tiles_w)

    rankers = n_pts + n_cand - 1
    awaited = (n_cand - 1) + rankers - jnp.where(ranks, 1, 0) + jnp.where(calls, n_pts - 1, 0)
    pl.semaphore_wait(barrier, awaited)
    early = sends(part_a, parts_a, a_send, a_recv)
    early.pop(0)()
    early.pop(0)()
    for at, (i, q) in enumerate(units):
        if at and at % 2 == 0:
            fence()
        consume(n_c - 1, i, q)
        for _ in range(-(-len(early) // (len(units) - at))):
            early.pop(0)()
    write_sums(n_c - 1, part_b, 0)
    for one in sends(part_b, parts_b, b_send, b_recv):
        one()
    pl.semaphore_wait(passed, len(fences))

    for r in range(0, rows, PIECE):
        at = slice(r, r + PIECE)
        cover_of([last[at, t * LANES : (t + 1) * LANES] for t in range(tiles_w)], at, n_c - 1)
    for t in range(tiles_p):
        turned = jnp.transpose(b_acc[t * LANES : (t + 1) * LANES, :])
        best[t : t + 1, :] = jnp.max(turned, axis=0, keepdims=True)
    for k in range(1, n_cand):
        pltpu.make_async_remote_copy(
            src_ref=best, dst_ref=bests.at[mz], send_sem=best_send.at[0], recv_sem=best_recv.at[0],
            device_id={"cand": lax.rem(mz + k, n_cand)}, device_id_type=MESH,
        ).start()

    def settle(view, sem):
        pltpu.make_async_copy(view, view, sem).wait()

    def finish_cover():
        settle(bests.at[pl.ds(0, n_cand - 1)], best_recv.at[0])
        cover = best[...]
        for k in range(1, n_cand):
            cover = jnp.maximum(cover, bests[lax.rem(mz + k, n_cand)])
        cover_out[...] = jnp.maximum(v_buf[...], cover * scale)
        settle(bests.at[pl.ds(0, n_cand - 1)], best_send.at[0])

    place = lax.broadcasted_iota(jnp.int32, (8, LANES), 1).astype(F32)
    lane = lax.broadcasted_iota(jnp.int32, (1, LANES), 1)

    def merge(new):
        for i, row in enumerate(new):
            n_col[i * LANES : (i + 1) * LANES, :] = column_tile(row)
        across = [jnp.broadcast_to(row, (8, LANES)) for row in new]
        across.append(jnp.broadcast_to(top_row[...], (8, LANES)))
        columns = [t_col[g * 8 : (g + 1) * 8, :] for g in range(TOPK // 8)]
        columns += [n_col[g * 8 : (g + 1) * 8, :] for g in range(len(new) * LANES // 8)]
        kept = jnp.full((8, LANES), HIGH, F32)
        for column in columns:
            above = jnp.zeros((8, LANES), F32)
            for row in across:
                above = above + jnp.where(row > column, 1.0, 0.0)
            above = jnp.sum(above, axis=1, keepdims=True)
            kept = jnp.minimum(kept, jnp.where(above <= place, column, HIGH))
        kept = jnp.min(kept, axis=0, keepdims=True)
        return jnp.where(lane < TOPK, kept, LOW)

    def told(p, src, dst, send, recv):
        return pltpu.make_async_remote_copy(
            src_ref=src, dst_ref=dst, send_sem=send.at[0], recv_sem=recv.at[0],
            device_id={"pts": p}, device_id_type=MESH,
        )

    def settle_either(fewer, view, many, sem):
        pl.when(fewer)(lambda: settle(view.at[pl.ds(0, many - 1)], sem))
        pl.when(jnp.logical_not(fewer))(lambda: settle(view.at[pl.ds(0, many)], sem))

    def settle_sends():
        settle_either(ranks, sent_a, rankers, a_send.at[0])
        settle_either(ranks, sent_b, rankers, b_send.at[0])

    def tell_all(src, dst, send, recv, here):
        def tell(k, carry):
            told(lax.rem(me + k, n_pts), src, dst, send, recv).start()
            return carry

        lax.fori_loop(1, jnp.where(here, n_pts, 1), tell, 0)

    def tell_gains(z):
        if z:
            tell_all(all_gains.at[z], got_gains, gain_send, gain_recv, calls & (mz == z))

    @pl.when(ranks)
    def _():
        top_row[...] = jnp.where(lane < TOPK, -1.0, LOW)
        for z in range(n_cand):
            for slots, recv, first, many in (
                (parts_a, a_recv, 0, rows_a), (parts_b, b_recv, rows_a, rows_b)
            ):
                if not first:
                    t_col[...] = column_tile(top_row[...])[:TOPK, :]
                settle_either(mz == z, slots.at[0], n_pts, recv.at[z])
                if first:
                    t_col[...] = column_tile(top_row[...])[:TOPK, :]
                total = slots[z, 0]
                for p in range(1, n_pts):
                    total = total + slots[z, p]
                all_gains[z, first : first + many, :] = total
                if first and z + 1 < n_cand:
                    tell_gains(z)
                if first and z + 1 == n_cand:
                    gains_out[...] = all_gains[mz]
                if first and z == max(n_cand - 2, 0):
                    finish_cover()
                    settle_sends()
                top_row[...] = merge([total[t : t + 1, :] for t in range(many)])
        top_out[...] = top_row[:, :TOPK]
        tell_all(top_row, got_top, top_send, top_recv, calls)
        tell_gains(n_cand - 1)

        def drain(k, carry):
            settle(heard, top_send.at[0])
            settle(sent, gain_send.at[0])
            return carry

        lax.fori_loop(0, jnp.where(calls, 1, 0), drain, 0)

    @pl.when(jnp.logical_not(ranks))
    def _():
        finish_cover()
        settle_sends()
        settle(got_gains, gain_recv.at[0])
        gains_out[...] = got_gains[...]
        settle(got_top, top_recv.at[0])
        top_out[...] = got_top[:, :TOPK]


def finish(gains, top, cover, gains_out, top_out, cover_out, sems):
    copies = [
        pltpu.make_async_copy(top, top_out, sems.at[0]),
        pltpu.make_async_copy(gains, gains_out, sems.at[1]),
        pltpu.make_async_copy(cover, cover_out, sems.at[2]),
    ]
    for copy in copies:
        copy.start()
    for copy in copies:
        copy.wait()


def solution(mesh):
    n_pts, n_cand = mesh.shape["pts"], mesh.shape["cand"]

    def on_device(points, weights, coverage, candidates, picks):
        rows, depth = points.shape
        cands = candidates.shape[0]
        tp, tc = rows // LANES, cands // LANES
        tb = WIDE // LANES
        ta = tc - tb
        anywhere = pl.BlockSpec(memory_space=pl.ANY)
        dma = pltpu.SemaphoreType.DMA
        vmem = pltpu.VMEM

        def scoped(*refs):
            many = rows // 2 // PIECE
            accs = [pltpu.ACC(q)((PIECE, WIDE), F32) for q in (0,) * many + (1,) * many] * 2
            pl.run_scoped(functools.partial(kernel, n_pts, n_cand, *refs), *accs)

        gains, top, cover = pl.pallas_call(
            scoped,
            out_shape=(vmem((tc, LANES), F32), vmem((1, TOPK), F32), vmem((tp, LANES), F32)),
            in_specs=[anywhere] * 5,
            out_specs=(pl.BlockSpec(memory_space=vmem),) * 3,
            scratch_shapes=[
                vmem((rows, depth), points.dtype), vmem((cands, depth), candidates.dtype),
                vmem((tp, LANES), F32), vmem((tp, LANES), F32),
                pltpu.SMEM(picks.shape, jnp.int32),
                vmem((rows, LANES), F32), vmem((rows, LANES), F32), vmem((rows, LANES), F32),
                vmem((rows, WIDE), F32),
                vmem((ta, LANES), F32), vmem((tb, LANES), F32),
                vmem((n_cand, n_pts, ta, LANES), F32), vmem((n_cand, n_pts, tb, LANES), F32),
                vmem((tp, LANES), F32), vmem((n_cand, tp, LANES), F32),
                vmem((n_cand, tc, LANES), F32), vmem((cands, LANES), F32), vmem((TOPK, LANES), F32),
                vmem((1, LANES), F32), vmem((tc, LANES), F32), vmem((1, LANES), F32),
                dma((depth // WIDE + 3,)), dma((3,)),
                dma((n_cand,)), dma((n_cand,)), dma((1,)), dma((1,)), dma((1,)),
                vmem((n_pts + n_cand - 1, ta, LANES), F32), vmem((n_pts + n_cand - 1, tb, LANES), F32),
                vmem((n_pts - 1, tc, LANES), F32), vmem((n_pts - 1, 1, LANES), F32),
                pltpu.SemaphoreType.REGULAR,
            ],
            compiler_params=pltpu.CompilerParams(
                collective_id=0, has_side_effects=True, vmem_limit_bytes=60 * 2**20,
            ),
            name="facility",
        )(points, weights.reshape(tp, LANES), coverage.reshape(tp, LANES), candidates, picks)
        gains, top, cover = pl.pallas_call(
            finish,
            out_shape=(
                jax.ShapeDtypeStruct((tc, LANES), F32),
                jax.ShapeDtypeStruct((1, TOPK), F32),
                jax.ShapeDtypeStruct((tp, LANES), F32),
            ),
            in_specs=[pl.BlockSpec(memory_space=vmem)] * 3,
            out_specs=(anywhere,) * 3,
            scratch_shapes=[dma((3,))],
            name="finish",
        )(*(pltpu.with_memory_space_constraint(x, vmem) for x in (gains, top, cover)))
        return gains.reshape(cands), top.reshape(TOPK), cover.reshape(rows)

    placed = (P("pts", None), P("pts"), P("pts"), P("cand", None), P())
    return jax.shard_map(
        on_device, mesh=mesh, in_specs=placed, out_specs=(P("cand"), P(), P("pts")), check_vma=False
    )
```
